256 devices in a mesh: prow: 16 (over x, y), pcol: 16 (over z, core).
Axes of the slice: x: 4, y: 4, z: 8, core: 2. Of those that a mesh axis runs over, the one named last changes fastest.
Arguments:
- matrix: float32 [16384, 16384], P('prow', 'pcol'), may hold values from -6 to 6
- pivots: int32 [2, 512], replicated, may hold values from 512 to 16383, as said below
- lower_inverses: float32 [2, 512, 512], replicated, as said below
- upper_inverses: float32 [2, 512, 512], replicated, as said below
Outputs:
- factored: float32 [16384, 16384], P('prow', 'pcol')
The draws below stay inside these ranges and needn't reach their ends.
Inputs may be any that keep to these rules, and one draw needn't show every extreme that they name: The 512 entries of pivots[j] are distinct and each is at least (j + 1) * 512. Each lower_inverses[j] is unit lower triangular. Each upper_inverses[j] is upper triangular with a positive diagonal.
All inputs are finite; a program needn't handle non-finite values.
Results may differ from the reference program's by a relative error of at most 0.0003.
Values sent between devices are 32-bit elements; how exact they have to be, the bound alone decides.
A program may use at most 128 MiB of HBM per device.

```python
import jax
import jax.numpy as jnp
from jax import lax

NB = 512
PANELS = 2
M = 16384
N_PROW = 16
N_PCOL = 16


def draw_pivots(key, part):
    listed = []
    for panel_step in range(PANELS):
        start_row = (panel_step + 1) * NB
        chosen = jax.random.permutation(jax.random.fold_in(key, panel_step + 11), M - start_row)[:NB]
        listed.append((chosen + start_row).astype(jnp.int32))
    return jnp.stack(listed)


def rough_entries(key):
    return jax.random.normal(key, (NB, NB), jnp.float32)


def draw_lower_inverses(key, part):
    listed = []
    for panel_step in range(PANELS):
        noise = rough_entries(jax.random.fold_in(key, panel_step + 21))
        listed.append(jnp.eye(NB, dtype=jnp.float32) + jnp.tril(noise, -1) * (0.7 / NB ** 0.5))
    return jnp.stack(listed)


def draw_upper_inverses(key, part):
    listed = []
    for panel_step in range(PANELS):
        noise = rough_entries(jax.random.fold_in(key, panel_step + 31))
        scales = jax.random.uniform(jax.random.fold_in(key, panel_step + 41), (NB,), jnp.float32, 0.5, 1.5)
        listed.append((jnp.diag(scales) + jnp.triu(noise, 1) * (0.7 / NB ** 0.5)) / NB ** 0.5)
    return jnp.stack(listed)


def block_levels(rng, shape, split, smallest, largest):
    def one(axis_at, blocks):
        heights = jax.random.uniform(jax.random.fold_in(jax.random.fold_in(rng, 6), axis_at), (blocks,), jnp.float32, smallest / len(split), largest / len(split))
        return jnp.repeat(jnp.exp(heights), shape[axis_at] // blocks).reshape((-1,) + (1,) * (len(shape) - axis_at - 1))

    loudness = one(*split[0])
    for cut in split[1:]:
        loudness = loudness * one(*cut)
    return loudness


def gaussian(rng, dims, deviation, bound, cuts=(), held_as=jnp.bfloat16):
    array = jax.random.normal(rng, dims, jnp.float32) * deviation
    if len(cuts) > 0:
        array = block_levels(rng, dims, cuts, -0.22, 0.18) * array
    return jnp.clip(array, min=-bound, max=bound).astype(held_as)


def setup_inputs(seed: int = 0) -> dict:
    key_list = jax.random.split(jax.random.key(seed), 5)
    return {
        "matrix": gaussian(key_list[0], (M, M), 1.0, 6.0, ((0, 16), (1, 16)), jnp.float32),
        "pivots": draw_pivots(jax.random.fold_in(key_list[4], 71), 0),
        "lower_inverses": draw_lower_inverses(jax.random.fold_in(key_list[4], 71), 0),
        "upper_inverses": draw_upper_inverses(jax.random.fold_in(key_list[4], 71), 0),
    }


def storage_order(count, parts):
    share = M // parts
    logical = jnp.arange(M, dtype=jnp.int32)
    blocks = logical // NB
    return ((blocks % parts) * share + (blocks // parts) * NB + logical % NB).astype(jnp.int32)


def reference(matrix, pivots, lower_inverses, upper_inverses):
    row_order = storage_order(M, N_PROW)
    col_order = storage_order(M, N_PCOL)
    logical = matrix[row_order][:, col_order]
    for panel_step in range(PANELS):
        start_col = panel_step * NB
        end_col = start_col + NB
        targets = pivots[panel_step].astype(jnp.int32)
        top_rows = logical[start_col:end_col]
        picked = logical[targets]
        logical = logical.at[targets].set(top_rows)
        logical = logical.at[start_col:end_col].set(picked)
        upper_part = jnp.dot(lower_inverses[panel_step], logical[start_col:end_col, end_col:], precision=lax.Precision.HIGHEST, preferred_element_type=jnp.float32)
        logical = logical.at[start_col:end_col, end_col:].set(upper_part)
        lower_part = jnp.dot(logical[end_col:, start_col:end_col], upper_inverses[panel_step], precision=lax.Precision.HIGHEST, preferred_element_type=jnp.float32)
        logical = logical.at[end_col:, start_col:end_col].set(lower_part)
        product = jnp.dot(lower_part, upper_part, precision=lax.Precision.HIGHEST, preferred_element_type=jnp.float32)
        logical = logical.at[end_col:, end_col:].add(-product)
    inverse_rows = jnp.zeros((M,), jnp.int32).at[row_order].set(jnp.arange(M, dtype=jnp.int32))
    inverse_cols = jnp.zeros((M,), jnp.int32).at[col_order].set(jnp.arange(M, dtype=jnp.int32))
    return logical[inverse_rows][:, inverse_cols]
```

```python
import functools

import jax
import jax.numpy as jnp
from jax import lax
from jax.experimental import pallas as pl
from jax.experimental.pallas import tpu as pltpu
from jax.sharding import PartitionSpec as P

NB = 512
CAP = 96
CHUNK = 32
BLOCK = CAP + 2 * CHUNK
ZROWS = 32
SKEW = 2
VM = pltpu.VMEM
SM = pltpu.SMEM
F32 = jnp.float32
BF16 = jnp.bfloat16


def spec(space):
    return pl.BlockSpec(memory_space=space)


def remote(src, dst, send, recv, where):
    return pltpu.make_async_remote_copy(
        src_ref=src, dst_ref=dst, send_sem=send, recv_sem=recv,
        device_id=where, device_id_type=pl.DeviceIdType.MESH,
    )


def tables(pivots, me):
    p0, p1 = pivots[0], pivots[1]
    i = jnp.arange(NB, dtype=jnp.int32)
    r = jnp.arange(2 * NB, dtype=jnp.int32)

    def held(rows, default):
        hit = jnp.max(jnp.where(rows[:, None] == p0[None, :], i[None, :] + 1, 0), axis=1)
        return jnp.where(hit > 0, hit - 1, default)

    t = jnp.concatenate([p0, held(p1, p1)])
    owner = (t >> 9) & 15
    local = ((t >> 13) << 9) | (t & 511)
    earlier = (owner[None, :] == owner[:, None]) & (r[None, :] < r[:, None])
    rank = jnp.sum(earlier.astype(jnp.int32), axis=1)
    k = jnp.arange(CAP, dtype=jnp.int32)
    mine = (owner == me)[None, :] & (rank[None, :] == k[:, None])
    pack = jnp.sum(jnp.where(mine, local[None, :], 0), axis=1)
    take = owner * BLOCK + rank
    second = held(i + NB, i + NB)
    g = (((r >> 9) << 4) + me) * NB + (r & 511)
    m1 = jnp.max(jnp.where(g[:, None] == p1[None, :], second[None, :] + 1, 0), axis=1)
    m0 = jnp.max(jnp.where(g[:, None] == p0[None, :], i[None, :] + 1, 0), axis=1)
    src = jnp.where(g < 2 * NB, -1, jnp.where(m1 > 0, m1, m0) - 1)
    old = jnp.where(
        src >= 0,
        ((src & 511) >> 5) * BLOCK + CAP + (src >> 9) * CHUNK + (src & 31),
        -1,
    )
    return pack, take, old, jnp.max(rank) < CAP


def gather_kernel(pack_ref, a_ref, g_ref, sta, stb, sc_send, sca_recv, scb_recv,
                  sc2_send, sc2_recv, loc_sem, ag_send, ag_recv):
    p = lax.axis_index("prow")
    x, y = p // 4, p % 4

    def at(px, py):
        return {"prow": px * 4 + py}

    def copy_row(k, carry):
        l = pack_ref[k]
        g_ref[p, pl.ds(k, 1), :] = a_ref[l // 128, (l // 32) % 4, pl.ds(l % 32, 1), :]
        return carry

    barrier = pltpu.get_barrier_semaphore()
    for d in (1, 2, 3):
        pl.semaphore_signal(barrier, inc=1, device_id=at((x + d) % 4, y),
                            device_id_type=pl.DeviceIdType.MESH)
        pl.semaphore_signal(barrier, inc=1, device_id=at(x, (y + d) % 4),
                            device_id_type=pl.DeviceIdType.MESH)
    lax.fori_loop(0, CAP, copy_row, 0)
    pl.semaphore_wait(barrier, 6)

    halves = (pl.ds(0, 512), pl.ds(512, 512))

    def old(panel):
        return pl.ds(CAP + panel * CHUNK, CHUNK)

    def first_a(panel, d):
        c = (x + d) % 4
        return remote(a_ref.at[c, :, :, halves[0]], sta, sc_send.at[d - 1],
                      sca_recv.at[0], at(c, y))

    def first_b(panel, d):
        c = (y + d) % 4
        return remote(a_ref.at[pl.ds(0, 4), c, :, halves[1]], stb.at[panel],
                      sc_send.at[d + 2], scb_recv.at[panel], at(x, c))

    def second_a(panel, d, src):
        c = (y + d) % 4
        return remote(src.at[c], g_ref.at[p // 4 * 4 + c, old(panel), halves[0]],
                      sc2_send.at[panel * 6 + d - 1], sc2_recv.at[panel * 2],
                      at(x, c))

    def second_b(panel, d, src):
        c = (x + d) % 4
        return remote(src.at[c], g_ref.at[c * 4 + y, old(panel), halves[1]],
                      sc2_send.at[panel * 6 + d + 2], sc2_recv.at[panel * 2 + 1],
                      at(c, y))

    def own(panel, half, src):
        return pltpu.make_async_copy(src, g_ref.at[p, old(panel), halves[half]],
                                     loc_sem.at[panel * 2 + half])

    for panel in range(2):
        @pl.when(p == panel)
        def _():
            for d in (2, 1, 3):
                first_a(panel, d).start()
                first_b(panel, d).start()
            for d in (2, 1, 3):
                second_a(panel, d, a_ref.at[0, :, :, halves[0]]).start()
                second_b(panel, d, a_ref.at[pl.ds(0, 4), panel, :, halves[1]]).start()
            own(panel, 0, a_ref.at[0, panel, :, halves[0]]).start()
            own(panel, 1, a_ref.at[0, panel, :, halves[1]]).start()

    def coords(half, du, dv):
        if half == 0:
            return (x + du) % 4, (y + dv) % 4
        return (x + dv) % 4, (y + du) % 4

    def ag(part, lo, n):
        m = n // 2

        def piece(half, du, dv, r0, rows):
            bx, by = coords(half, du, dv)
            return g_ref.at[bx * 4 + by, pl.ds(lo + r0, rows), halves[half]]

        def cp(half, slot, du, dv, r0, rows, tu, tv):
            ref = piece(half, du, dv, r0, rows)
            s = (part * 2 + half) * 20 + slot
            return remote(ref, ref, ag_send.at[s], ag_recv.at[s], at(*coords(half, tu, tv)))

        def st1(half, which):
            return cp(half, which, *(
                (0, 0, 0, n, 1, 0),
                (0, 0, 0, n, 3, 0),
                (3, 0, 0, m, 1, 0),
                (1, 0, m, m, 3, 0),
            )[which])

        shift = (0, 3, 1, 2)

        def st2(half, j, which):
            u = shift[j]
            s = 4 + j * 4
            return cp(half, s + which, *(
                (u, 0, 0, n, 0, 1),
                (u, 0, 0, n, 0, 3),
                (u, 3, 0, m, 0, 1),
                (u, 1, m, m, 0, 3),
            )[which])

        hs = (0, 1)
        for h in hs:
            st1(h, 0).start()
            st1(h, 1).start()
        for h in hs:
            st2(h, 0, 0).start()
            st2(h, 0, 1).start()
        yield
        for h in hs:
            st1(h, 0).wait_recv()
            st1(h, 2).start()
            st1(h, 1).wait_recv()
            st1(h, 3).start()
        for h in hs:
            for j in (1, 2):
                st2(h, j, 0).start()
                st2(h, j, 1).start()
        for h in hs:
            st1(h, 2).wait_recv()
            st1(h, 3).wait_recv()
            st2(h, 3, 0).start()
            st2(h, 3, 1).start()
        yield
        for j in range(4):
            for h in hs:
                st2(h, j, 0).wait_recv()
                st2(h, j, 2).start()
                st2(h, j, 1).wait_recv()
                st2(h, j, 3).start()
        yield
        for j in range(4):
            for h in hs:
                st2(h, j, 2).wait_recv()
                st2(h, j, 3).wait_recv()
        for h in hs:
            for w in range(4):
                st1(h, w).wait_send()
                for j in range(4):
                    st2(h, j, w).wait_send()
        yield

    packed = ag(0, 0, CAP)
    next(packed)

    for panel in range(2):
        @pl.when((y == panel) & (x != 0))
        def _():
            first_a(panel, 1).wait_recv()
            for d in (2, 1, 3):
                second_a(panel, d, sta).start()
            own(panel, 0, sta.at[panel]).start()

        @pl.when((x == 0) & (y != panel))
        def _():
            first_b(panel, 1).wait_recv()
            for d in (2, 1, 3):
                second_b(panel, d, stb.at[panel]).start()
            own(panel, 1, stb.at[panel, 0]).start()

    next(packed)

    for panel in range(2):
        @pl.when(y == panel)
        def _():
            own(panel, 0, sta.at[panel]).wait()

        @pl.when(y != panel)
        def _():
            second_a(panel, 1, sta).wait_recv()

        @pl.when(x == 0)
        def _():
            own(panel, 1, stb.at[panel, 0]).wait()

        @pl.when(x != 0)
        def _():
            second_b(panel, 1, stb.at[panel]).wait_recv()

    oldrows = ag(1, CAP, 2 * CHUNK)
    next(oldrows)
    next(packed)
    next(oldrows)
    next(packed)
    next(oldrows)
    next(oldrows)

    for panel in range(2):
        @pl.when(p == panel)
        def _():
            for d in (1, 2, 3):
                first_a(panel, d).wait_send()
                first_b(panel, d).wait_send()

        @pl.when(y == panel)
        def _():
            for d in (1, 2, 3):
                second_a(panel, d, sta).wait_send()

        @pl.when(x == 0)
        def _():
            for d in (1, 2, 3):
                second_b(panel, d, stb.at[panel]).wait_send()


def gather_rows(pack, matrix):
    return pl.pallas_call(
        gather_kernel,
        out_shape=jax.ShapeDtypeStruct((16, BLOCK, 1024), F32),
        in_specs=[spec(SM), spec(VM)],
        out_specs=spec(VM),
        scratch_shapes=[
            VM((4, CHUNK, 512), F32),
            VM((2, 4, CHUNK, 512), F32),
            pltpu.SemaphoreType.DMA((6,)),
            pltpu.SemaphoreType.DMA((1,)),
            pltpu.SemaphoreType.DMA((2,)),
            pltpu.SemaphoreType.DMA((12,)),
            pltpu.SemaphoreType.DMA((4,)),
            pltpu.SemaphoreType.DMA((4,)),
            pltpu.SemaphoreType.DMA((80,)),
            pltpu.SemaphoreType.DMA((80,)),
        ],
        compiler_params=pltpu.CompilerParams(collective_id=0, has_side_effects=True),
        name="gather_rows",
    )(pack, matrix.reshape(8, 4, CHUNK, 1024))


def unpack_kernel(take_ref, old_ref, a_ref, g_ref, b_ref, t_ref, z_ref):
    c = lax.axis_index("pcol")

    def top(r, carry):
        t_ref[pl.ds(r, 1), :] = g_ref[pl.ds(take_ref[r], 1), :]
        return carry

    lax.fori_loop(0, 2 * NB, top, 0, unroll=8)
    b_ref[...] = a_ref[...]

    def swap(r, carry):
        s = old_ref[r]

        @pl.when(s >= 0)
        def _():
            b_ref[pl.ds(r, 1), :] = g_ref[pl.ds(s, 1), :]

        return carry

    lax.fori_loop(0, 2 * NB, swap, 0, unroll=8)

    @pl.when(c < 2)
    def _():
        z_ref[0:1024, :] = b_ref[:, 0:NB]

    @pl.when(c == 0)
    def _():
        z_ref[1024:1536, :] = t_ref[NB:, 0:NB]

    @pl.when(c == 1)
    def _():
        z_ref[1024:1536, :] = t_ref[0:NB, 0:NB]


def unpack(take, old, matrix, gathered):
    return pl.pallas_call(
        unpack_kernel,
        out_shape=(
            jax.ShapeDtypeStruct((1024, 1024), F32),
            jax.ShapeDtypeStruct((1024, 1024), F32),
            jax.ShapeDtypeStruct((1536, NB), F32),
        ),
        in_specs=[spec(SM), spec(SM), spec(VM), spec(VM)],
        out_specs=(spec(VM), spec(VM), spec(VM)),
        name="unpack",
    )(take, old, matrix, gathered.reshape(16 * BLOCK, 1024))


def cast_kernel(n, z_ref, o_ref, up_send, up_recv, dn_send, dn_recv, sib_send, sib_recv, loc):
    c = lax.axis_index("pcol")
    z, core = c // 2, c % 2

    def at(pz, pc):
        return {"pcol": pz * 2 + pc}

    barrier = pltpu.get_barrier_semaphore()
    for dev in (at((z + 1) % 8, core), at((z + 7) % 8, core), at(z, 1 - core)):
        pl.semaphore_signal(barrier, inc=1, device_id=dev, device_id_type=pl.DeviceIdType.MESH)
    pl.semaphore_wait(barrier, 3)

    def rows(k):
        return pl.ds(pl.multiple_of(k * ZROWS, ZROWS), ZROWS)

    def hop(src, k, up):
        if up:
            return remote(src.at[rows(k)], o_ref.at[core, rows(k)], up_send.at[k],
                          up_recv.at[k], at((z + 1) % 8, core))
        return remote(src.at[rows(n + k)], o_ref.at[core, rows(n + k)], dn_send.at[k],
                      dn_recv.at[k], at((z + 7) % 8, core))

    def sib(src, k):
        return remote(src.at[rows(k)], o_ref.at[core, rows(k)], sib_send.at[k],
                      sib_recv.at[k], at(z, 1 - core))

    mine = o_ref.at[core]

    @pl.when(z == 0)
    def _():
        def step(k, carry):
            hop(z_ref, k, True).start()
            hop(z_ref, k, False).start()
            return carry
        lax.fori_loop(0, n, step, 0)

        def side(k, carry):
            sib(z_ref, k).start()
            return carry
        lax.fori_loop(0, 2 * n, side, 0)
        keep = pltpu.make_async_copy(z_ref, mine, loc)
        keep.start()
        keep.wait()

        def done(k, carry):
            hop(z_ref, k, True).wait_send()
            hop(z_ref, k, False).wait_send()
            return carry
        lax.fori_loop(0, n, done, 0)

    @pl.when(z != 0)
    def _():
        def step(t, carry):
            k0 = t - SKEW * z
            k1 = t - SKEW * (8 - z)

            @pl.when((k0 >= 0) & (k0 < n))
            def _():
                hop(mine, k0, True).wait_recv()

                @pl.when(z < 7)
                def _():
                    hop(mine, k0, True).start()
                sib(mine, k0).start()

            @pl.when((k1 >= 0) & (k1 < n))
            def _():
                hop(mine, k1, False).wait_recv()

                @pl.when(z > 1)
                def _():
                    hop(mine, k1, False).start()
                sib(mine, n + k1).start()
            return carry
        lax.fori_loop(SKEW, n + 7 * SKEW, step, 0)

        @pl.when(z < 7)
        def _():
            def done(k, carry):
                hop(mine, k, True).wait_send()
                return carry
            lax.fori_loop(0, n, done, 0)

        @pl.when(z > 1)
        def _():
            def done(k, carry):
                hop(mine, k, False).wait_send()
                return carry
            lax.fori_loop(0, n, done, 0)

    other = o_ref.at[1 - core]

    def finish(k, carry):
        sib(mine, k).wait_send()
        remote(other.at[rows(k)], other.at[rows(k)], sib_send.at[k], sib_recv.at[k],
               at(z, 1 - core)).wait_recv()
        return carry
    lax.fori_loop(0, 2 * n, finish, 0)


def broadcast_z(panel):
    n = panel.shape[0] // (2 * ZROWS)
    dma = pltpu.SemaphoreType.DMA
    return pl.pallas_call(
        functools.partial(cast_kernel, n),
        out_shape=jax.ShapeDtypeStruct((2,) + panel.shape, F32),
        in_specs=[spec(VM)],
        out_specs=spec(VM),
        scratch_shapes=[dma((n,)), dma((n,)), dma((n,)), dma((n,)),
                        dma((2 * n,)), dma((2 * n,)), dma],
        compiler_params=pltpu.CompilerParams(collective_id=1, has_side_effects=True),
        name="broadcast_z",
    )(panel)


def split(v):
    hi = v.astype(BF16)
    return hi, (v - hi.astype(F32)).astype(BF16)


def dot3(a, b):
    f = functools.partial(jnp.dot, preferred_element_type=F32)
    return f(a[0], b[0]) + (f(a[0], b[1]) + f(a[1], b[0]))


def put(ref, rows, cols, v):
    hi, lo = split(v)
    ref[0, rows, cols] = hi
    ref[1, rows, cols] = lo


def get(ref, rows, cols):
    return ref[0, rows, cols], ref[1, rows, cols]


def update_kernel(b_ref, t_ref, pp_ref, li_ref, ui_ref, f_ref, u_s, l_s, uc_s, li_s, ui_s):
    p = lax.axis_index("prow")
    c = lax.axis_index("pcol")
    full = pl.ds(0, NB)

    def tile(i, size=256):
        return pl.ds(pl.multiple_of(i * size, size), size)

    for j in range(2):
        li_s[2 * j], li_s[2 * j + 1] = split(li_ref[j])
        ui_s[2 * j], ui_s[2 * j + 1] = split(ui_ref[j])

    def inv(ref, j, rows, cols):
        return ref[2 * j, rows, cols], ref[2 * j + 1, rows, cols]

    @pl.loop(0, 2)
    def _(i):
        put(uc_s, full, tile(i), dot3(inv(li_s, 0, full, full), split(pp_ref[1, 1024:1536, tile(i)])))

    @pl.loop(0, 6)
    def _(i):
        put(l_s, tile(i), full, dot3(split(pp_ref[0, tile(i), :]), inv(ui_s, 0, full, full)))

    @pl.loop(0, 4)
    def _(i):
        left = get(l_s, tile(i), full)
        rest = pp_ref[1, tile(i), :] - dot3(left, get(uc_s, full, full))
        put(l_s, tile(i), pl.ds(NB, NB), dot3(split(rest), inv(ui_s, 1, full, full)))

    @pl.loop(0, 4)
    def _(i):
        cols = tile(i)
        u0 = dot3(inv(li_s, 0, full, full), split(t_ref[0:NB, cols]))
        put(u_s, full, cols, u0)
        t1 = t_ref[NB:, cols] - dot3(get(l_s, pl.ds(1024, NB), full), get(u_s, full, cols))
        u1 = dot3(inv(li_s, 1, full, full), split(t1))
        put(u_s, pl.ds(NB, NB), cols, u1)

        @pl.loop(0, 4)
        def _(k):
            rows = tile(k)
            f_ref[rows, cols] = b_ref[rows, cols] - dot3(
                get(l_s, rows, pl.ds(0, 2 * NB)), get(u_s, pl.ds(0, 2 * NB), cols))

        @pl.when(p == 0)
        def _():
            f_ref[0:NB, cols] = u0

            @pl.when((c == 0) & (i < 2))
            def _():
                f_ref[0:NB, cols] = t_ref[0:NB, cols]

        @pl.when(p == 1)
        def _():
            f_ref[0:NB, cols] = u1

            @pl.when((c == 1) & (i < 2))
            def _():
                f_ref[0:NB, cols] = t1

    def lower(src, dst, part):
        f_ref[dst, 0:NB] = (l_s[0, src, part].astype(F32) + l_s[1, src, part].astype(F32))

    for j in range(2):
        part = pl.ds(j * NB, NB)

        @pl.when(c == j)
        def _():
            lower(pl.ds(NB, NB), pl.ds(NB, NB), part)

            @pl.when(p > j)
            def _():
                lower(full, full, part)

    @pl.when((c == 0) & (p == 1))
    def _():
        lower(pl.ds(1024, NB), full, full)


def update(b, t, pp, li, ui):
    return pl.pallas_call(
        update_kernel,
        out_shape=jax.ShapeDtypeStruct((1024, 1024), F32),
        in_specs=[spec(VM)] * 5,
        out_specs=spec(VM),
        scratch_shapes=[
            VM((2, 1024, 1024), BF16),
            VM((2, 1536, 1024), BF16),
            VM((2, NB, NB), BF16),
            VM((4, NB, NB), BF16),
            VM((4, NB, NB), BF16),
        ],
        name="update",
    )(b, t, pp, li, ui)


def spread(value, axis, source):
    kept = jnp.where(lax.axis_index(axis) == source, value, 0).astype(value.dtype)
    return lax.psum(kept, axis)


def general(matrix, pivots, lower_inverses, upper_inverses):
    my_row = lax.axis_index("prow")
    my_col = lax.axis_index("pcol")
    rows_local, cols_local = matrix.shape
    dot = functools.partial(jnp.dot, precision=lax.Precision.HIGH, preferred_element_type=F32)
    row_blocks = jnp.arange(rows_local, dtype=jnp.int32) // NB * 16 + my_row
    col_blocks = jnp.arange(cols_local, dtype=jnp.int32) // NB * 16 + my_col

    def panel(step, current):
        targets = pivots[step]
        blocks = targets // NB
        slot = blocks // 16 * NB + targets % NB
        is_mine = blocks % 16 == my_row
        picked = jnp.where(is_mine[:, None], current[slot], 0.0)
        old_top = spread(current[:NB], "prow", step)
        new_top = lax.psum(picked, "prow")
        after = (col_blocks > step)[None, :]
        top = jnp.where(after, dot(lower_inverses[step], new_top), new_top)
        current = current.at[jnp.where(is_mine, slot, rows_local)].set(old_top, mode="drop")
        current = current.at[:NB].set(jnp.where(my_row == step, top, current[:NB]))
        column = spread(current[:, :NB], "pcol", step)
        below = (row_blocks > step)[:, None]
        lower = jnp.where(below, dot(column, upper_inverses[step]), 0.0)
        current = current - dot(lower, jnp.where(after, top, 0.0))
        return current.at[:, :NB].set(
            jnp.where(below & (my_col == step), lower, current[:, :NB]))

    return lax.fori_loop(0, 2, panel, matrix)


def fast(matrix, pack, take, old, li, ui):
    gathered = gather_rows(pack, matrix)
    b, t, z = unpack(take, old, matrix, gathered)
    return update(b, t, broadcast_z(z), li, ui)


def body(matrix, pivots, lower_inverses, upper_inverses):
    pack, take, old, fits = tables(pivots, lax.axis_index("prow"))
    return lax.cond(
        fits,
        lambda: fast(matrix, pack, take, old, lower_inverses, upper_inverses),
        lambda: general(matrix, pivots, lower_inverses, upper_inverses),
    )


def solution(mesh):
    placed = (P("prow", "pcol"), P(), P(), P())
    return jax.shard_map(
        body, mesh=mesh, in_specs=placed, out_specs=P("prow", "pcol"), check_vma=False
    )
```

```python
import functools

import jax
import jax.numpy as jnp
from jax import lax
from jax.experimental import pallas as pl
from jax.experimental.pallas import tpu as pltpu
from jax.sharding import PartitionSpec as P

NB = 512
CAP = 96
CHUNK = 32
HALF = CAP // 2
ZROWS = 16
ROWS = 768 + HALF
STREAM = ROWS // ZROWS
SKEW = 5
VM = pltpu.VMEM
SM = pltpu.SMEM
F32 = jnp.float32
BF16 = jnp.bfloat16


def spec(space):
    return pl.BlockSpec(memory_space=space)


def remote(src, dst, send, recv, where):
    return pltpu.make_async_remote_copy(
        src_ref=src, dst_ref=dst, send_sem=send, recv_sem=recv,
        device_id=where, device_id_type=pl.DeviceIdType.MESH,
    )


def tables(pivots, me):
    p0, p1 = pivots[0], pivots[1]
    i = jnp.arange(NB, dtype=jnp.int32)
    r = jnp.arange(2 * NB, dtype=jnp.int32)

    def held(rows, default):
        hit = jnp.max(jnp.where(rows[:, None] == p0[None, :], i[None, :] + 1, 0), axis=1)
        return jnp.where(hit > 0, hit - 1, default)

    t = jnp.concatenate([p0, held(p1, p1)])
    owner = (t >> 9) & 15
    local = ((t >> 13) << 9) | (t & 511)
    earlier = (owner[None, :] == owner[:, None]) & (r[None, :] < r[:, None])
    rank = jnp.sum(earlier.astype(jnp.int32), axis=1)
    k = jnp.arange(CAP, dtype=jnp.int32)
    mine = (owner == me)[None, :] & (rank[None, :] == k[:, None])
    pack = jnp.sum(jnp.where(mine, local[None, :], 0), axis=1)
    take = owner * 256 + rank
    second = held(i + NB, i + NB)
    g = (((r >> 9) << 4) + me) * NB + (r & 511)
    m1 = jnp.max(jnp.where(g[:, None] == p1[None, :], second[None, :] + 1, 0), axis=1)
    m0 = jnp.max(jnp.where(g[:, None] == p0[None, :], i[None, :] + 1, 0), axis=1)
    src = jnp.where(g < 2 * NB, -1, jnp.where(m1 > 0, m1, m0) - 1)
    valid = src >= 0
    count = jnp.sum((valid[None, :] & (r[None, :] < r[:, None])).astype(jnp.int32), axis=1)
    chosen = valid[None, :] & (count[None, :] == k[:, None])
    cpos = jnp.sum(jnp.where(chosen, r[None, :], 0), axis=1)
    csrc = ((src & 511) >> 5) * 256 + (src >> 9) * CHUNK + (src & 31)
    csrc = jnp.sum(jnp.where(chosen, csrc[None, :], 0), axis=1)
    total = jnp.sum(valid.astype(jnp.int32)).reshape(1)
    return pack, take, csrc, cpos, total, jnp.max(rank) < CAP


def split(v):
    hi = v.astype(BF16)
    return hi, (v - hi.astype(F32)).astype(BF16)


def dot3(a, b):
    f = functools.partial(jnp.dot, preferred_element_type=F32)
    return f(a[0], b[0]) + (f(a[0], b[1]) + f(a[1], b[0]))


def put(ref, rows, cols, v):
    hi, lo = split(v)
    ref[0, rows, cols] = hi
    ref[1, rows, cols] = lo


def get(ref, rows, cols):
    return ref[0, rows, cols], ref[1, rows, cols]


def factor_kernel(pack_ref, take_ref, csrc_ref, a_ref, li_ref, ui_ref, f_ref, fc_ref,
                  sa_ref, oa_ref, sb_ref, ob_ref, pp_ref, t_ref, u_s, l_s, uc_s, li_s, ui_s, sta, stb,
                  sc_send, sca_recv, scb_recv, sc2_send, sc2_recv, loc_sem,
                  ag_send, ag_recv,
                  up_send, up_recv, dn_send, dn_recv, sib_send, sib_recv):
    p = lax.axis_index("prow")
    x, y = p // 4, p % 4
    c = lax.axis_index("pcol")
    z, core = c // 2, c % 2

    def at(px, py):
        return {"prow": px * 4 + py}

    def zat(pz, pc):
        return {"pcol": pz * 2 + pc}

    def signal(sem, where):
        pl.semaphore_signal(sem, inc=1, device_id=where,
                            device_id_type=pl.DeviceIdType.MESH)

    barrier = pltpu.get_barrier_semaphore()
    for d in (1, 2, 3):
        signal(barrier, at((x + d) % 4, y))
        signal(barrier, at(x, (y + d) % 4))
    signal(barrier, zat((z + 1) % 8, core))
    signal(barrier, zat((z + 7) % 8, core))
    signal(barrier, zat(z, 1 - core))

    def packed_row(k, carry):
        l = pack_ref[k]
        row = a_ref[l // 128, (l // 32) % 4, pl.ds(l % 32, 1), :]
        sa_ref[p, pl.ds(k, 1), :] = row[:, 0:NB]
        sb_ref[p, pl.ds(k, 1), :] = row[:, NB:]
        return carry

    lax.fori_loop(0, CAP, packed_row, 0, unroll=4)

    @pl.when(z == 0)
    def _():
        @pl.loop(0, 32)
        def _(i):
            pp_ref[core, i // 16, pl.ds(pl.multiple_of(i % 16 * 32, 32), 32), :] = (
                a_ref[i // 4, i % 4, :, 0:NB])

    for j in range(2):
        li_s[2 * j], li_s[2 * j + 1] = split(li_ref[j])
        ui_s[2 * j], ui_s[2 * j + 1] = split(ui_ref[j])

    pl.semaphore_wait(barrier, 9)

    def quarter(i):
        return pl.ds(256 * i, 256)

    packed, olds = (sa_ref, sb_ref), (oa_ref, ob_ref)

    def old(panel):
        return pl.ds(panel * CHUNK, CHUNK)

    def first_a(ab, panel, d):
        k = (x + d) % 4
        return remote(a_ref.at[k, :, :, quarter(2 * ab)], sta.at[ab],
                      sc_send.at[ab * 6 + d - 1], sca_recv.at[ab], at(k, y))

    def first_b(ab, panel, d):
        k = (y + d) % 4
        return remote(a_ref.at[pl.ds(0, 4), k, :, quarter(2 * ab + 1)], stb.at[ab, panel],
                      sc_send.at[ab * 6 + d + 2], scb_recv.at[ab * 2 + panel], at(x, k))

    def second_a(ab, panel, d, src):
        k = (y + d) % 4
        return remote(src.at[k], olds[ab].at[x * 4 + k, old(panel), quarter(0)],
                      sc2_send.at[ab * 12 + panel * 6 + d - 1],
                      sc2_recv.at[ab * 4 + panel * 2], at(x, k))

    def second_b(ab, panel, d, src):
        k = (x + d) % 4
        return remote(src.at[k], olds[ab].at[k * 4 + y, old(panel), quarter(1)],
                      sc2_send.at[ab * 12 + panel * 6 + d + 2],
                      sc2_recv.at[ab * 4 + panel * 2 + 1], at(k, y))

    def own(ab, panel, half, src):
        return pltpu.make_async_copy(src, olds[ab].at[p, old(panel), quarter(half)],
                                     loc_sem.at[ab * 4 + panel * 2 + half])

    def scatter(ab):
        qa, qb = quarter(2 * ab), quarter(2 * ab + 1)
        for panel in range(2):
            @pl.when(p == panel)
            def _():
                for d in (2, 1, 3):
                    first_a(ab, panel, d).start()
                    first_b(ab, panel, d).start()
                for d in (2, 1, 3):
                    second_a(ab, panel, d, a_ref.at[0, :, :, qa]).start()
                    second_b(ab, panel, d, a_ref.at[pl.ds(0, 4), panel, :, qb]).start()
                own(ab, panel, 0, a_ref.at[0, panel, :, qa]).start()
                own(ab, panel, 1, a_ref.at[0, panel, :, qb]).start()

    def relay(ab):
        for panel in range(2):
            @pl.when((y == panel) & (x != 0))
            def _():
                first_a(ab, panel, 1).wait_recv()
                for d in (2, 1, 3):
                    second_a(ab, panel, d, sta.at[ab]).start()
                own(ab, panel, 0, sta.at[ab, panel]).start()

            @pl.when((x == 0) & (y != panel))
            def _():
                first_b(ab, panel, 1).wait_recv()
                for d in (2, 1, 3):
                    second_b(ab, panel, d, stb.at[ab, panel]).start()
                own(ab, panel, 1, stb.at[ab, panel, 0]).start()

    def scattered(ab):
        for panel in range(2):
            @pl.when(y == panel)
            def _():
                own(ab, panel, 0, sta.at[ab, panel]).wait()

            @pl.when(y != panel)
            def _():
                second_a(ab, panel, 1, sta.at[ab]).wait_recv()

            @pl.when(x == 0)
            def _():
                own(ab, panel, 1, stb.at[ab, panel, 0]).wait()

            @pl.when(x != 0)
            def _():
                second_b(ab, panel, 1, stb.at[ab, panel]).wait_recv()

    def scatter_drain(ab):
        for panel in range(2):
            @pl.when(p == panel)
            def _():
                for d in (1, 2, 3):
                    first_a(ab, panel, d).wait_send()
                    first_b(ab, panel, d).wait_send()

            @pl.when(y == panel)
            def _():
                for d in (1, 2, 3):
                    second_a(ab, panel, d, sta.at[ab]).wait_send()

            @pl.when(x == 0)
            def _():
                for d in (1, 2, 3):
                    second_b(ab, panel, d, stb.at[ab, panel]).wait_send()

    def coords(half, du, dv):
        if half == 0:
            return (x + du) % 4, (y + dv) % 4
        return (x + dv) % 4, (y + du) % 4

    shift = (0, 3, 1, 2)
    hs = (0, 1)

    def all_gather(ab, kind):
        n = (CAP, 2 * CHUNK)[kind]
        buffer = (packed, olds)[kind][ab]
        m = n // 2
        part = ab * 2 + kind

        def cp(half, slot, du, dv, r0, rows, tu, tv):
            bx, by = coords(half, du, dv)
            ref = buffer.at[bx * 4 + by, pl.ds(r0, rows), quarter(half)]
            s = (part * 2 + half) * 20 + slot
            return remote(ref, ref, ag_send.at[s], ag_recv.at[s], at(*coords(half, tu, tv)))

        def st1(half, which):
            return cp(half, which, *(
                (0, 0, 0, n, 1, 0),
                (0, 0, 0, n, 3, 0),
                (3, 0, 0, m, 1, 0),
                (1, 0, m, m, 3, 0),
            )[which])

        def st2(half, j, which):
            u = shift[j]
            return cp(half, 4 + j * 4 + which, *(
                (u, 0, 0, n, 0, 1),
                (u, 0, 0, n, 0, 3),
                (u, 3, 0, m, 0, 1),
                (u, 1, m, m, 0, 3),
            )[which])

        for h in hs:
            st1(h, 0).start()
            st1(h, 1).start()
        for h in hs:
            st2(h, 0, 0).start()
            st2(h, 0, 1).start()
        yield
        for h in hs:
            st1(h, 0).wait_recv()
            st1(h, 2).start()
            st1(h, 1).wait_recv()
            st1(h, 3).start()
        for h in hs:
            for j in (1, 2):
                st2(h, j, 0).start()
                st2(h, j, 1).start()
        yield
        for h in hs:
            st1(h, 2).wait_recv()
            st1(h, 3).wait_recv()
            st2(h, 3, 0).start()
            st2(h, 3, 1).start()
        yield
        for j in range(4):
            for h in hs:
                st2(h, j, 0).wait_recv()
                st2(h, j, 2).start()
                st2(h, j, 1).wait_recv()
                st2(h, j, 3).start()
        yield
        for j in range(4):
            for h in hs:
                st2(h, j, 2).wait_recv()
                st2(h, j, 3).wait_recv()
        yield
        for h in hs:
            for w in range(4):
                st1(h, w).wait_send()
                for j in range(4):
                    st2(h, j, w).wait_send()
        yield

    def rows(k):
        return pl.ds(pl.multiple_of(k * ZROWS, ZROWS), ZROWS)

    def hop(k, d):
        ref = pp_ref.at[core, d, rows(k)]
        if d == 0:
            return remote(ref, ref, up_send.at[k], up_recv.at[k], zat((z + 1) % 8, core))
        return remote(ref, ref, dn_send.at[k], dn_recv.at[k], zat((z + 7) % 8, core))

    def sib(k, d, which):
        ref = pp_ref.at[which, d, rows(k)]
        s = d * STREAM + k
        return remote(ref, ref, sib_send.at[s], sib_recv.at[s], zat(z, 1 - core))

    def z_source(k0, k1):
        def step(k, carry):
            for d in (0, 1):
                hop(k, d).start()
            for d in (0, 1):
                sib(k, d, core).start()
            return carry
        lax.fori_loop(k0, k1, step, 0)

    def z_relay(t0, t1):
        @pl.when(z != 0)
        def _():
            def step(t, carry):
                for d in (0, 1):
                    k = t - SKEW * (z if d == 0 else 8 - z)

                    @pl.when((k >= 0) & (k < STREAM))
                    def _():
                        hop(k, d).wait_recv()

                        @pl.when(z != (7 if d == 0 else 1))
                        def _():
                            hop(k, d).start()
                        sib(k, d, core).start()
                return carry
            lax.fori_loop(t0, t1, step, 0)

    def z_finish():
        def got(k, carry):
            for d in (0, 1):
                sib(k, d, 1 - core).wait_recv()
            return carry
        lax.fori_loop(0, STREAM, got, 0)

    def z_drain():
        def sent(k, carry):
            for d in (0, 1):
                sib(k, d, core).wait_send()

                @pl.when(z != (7 if d == 0 else 1))
                def _():
                    hop(k, d).wait_send()
            return carry
        lax.fori_loop(0, STREAM, sent, 0)

    def landed(buffer, v):
        return buffer[v // 256, pl.ds(v % 256, 1), :]

    left, right = pl.ds(0, NB), pl.ds(NB, NB)

    def panel_tops():
        @pl.when(z == 0)
        def _():
            def one(r, carry):
                v = take_ref[r + NB * (1 - core)]
                pp_ref[core, r // 256, pl.ds(NB + r % 256, 1), :] = landed(sa_ref, v)
                return carry
            lax.fori_loop(0, NB, one, 0, unroll=8)
            z_source(32, 48)

    def panel_swapped():
        @pl.when(z == 0)
        def _():
            def one(k, carry):
                pp_ref[core, k // HALF, pl.ds(768 + k % HALF, 1), :] = landed(oa_ref, csrc_ref[k])
                return carry
            lax.fori_loop(0, CAP, one, 0, unroll=8)
            z_source(48, STREAM)

    sa, oa = all_gather(0, 0), all_gather(0, 1)
    sb, ob = all_gather(1, 0), all_gather(1, 1)
    next(sa)
    scatter(0)
    scatter(1)

    @pl.when(z == 0)
    def _():
        z_source(0, 32)

    z_relay(5, 8)
    next(sa)
    z_relay(8, 13)
    next(sa)
    relay(0)
    z_relay(13, 20)
    relay(1)
    next(sb)
    z_relay(20, 26)
    next(sa)
    scattered(0)
    next(oa)
    z_relay(26, 32)
    next(oa)
    z_relay(32, 36)
    next(oa)
    next(sa)
    panel_tops()
    z_relay(36, 44)
    next(oa)
    next(sb)
    z_relay(44, 50)
    next(oa)
    panel_swapped()
    next(sb)
    scattered(1)
    next(ob)
    z_relay(50, 60)
    next(sb)
    next(ob)
    z_relay(60, 68)
    next(ob)
    next(sb)
    z_relay(68, STREAM + 7 * SKEW)
    next(ob)
    z_finish()

    full = pl.ds(0, NB)

    def tile(i, size=256):
        return pl.ds(pl.multiple_of(i * size, size), size)

    def lrow(d, r, n):
        return pl.ds(pl.multiple_of(d * ROWS + r, 16), n)

    def inv(ref, j, r, k):
        return ref[2 * j, r, k], ref[2 * j + 1, r, k]

    def top_row(r, carry):
        v = take_ref[r]
        t_ref[pl.ds(r, 1), left] = landed(sa_ref, v)
        t_ref[pl.ds(r, 1), right] = landed(sb_ref, v)
        return carry

    lax.fori_loop(0, 2 * NB, top_row, 0, unroll=8)

    def lower0(d, r, n):
        src = pl.ds(pl.multiple_of(r, 16), n)
        put(l_s, lrow(d, r, n), full, dot3(split(pp_ref[0, d, src, :]), inv(ui_s, 0, full, full)))

    def lower1(d, r, n):
        src = pl.ds(pl.multiple_of(r, 16), n)
        rest = pp_ref[1, d, src, :] - dot3(get(l_s, lrow(d, r, n), full), get(uc_s, full, full))
        put(l_s, lrow(d, r, n), pl.ds(NB, NB), dot3(split(rest), inv(ui_s, 1, full, full)))

    @pl.loop(0, 2)
    def _(i):
        uc = sum(
            dot3(inv(li_s, 0, full, tile(d)), split(pp_ref[1, d, pl.ds(NB, 256), tile(i)]))
            for d in (0, 1)
        )
        put(uc_s, full, tile(i), uc)

    @pl.loop(0, 6)
    def _(i):
        lower0(i // 3, i % 3 * 256, 256)

    @pl.loop(0, 4)
    def _(i):
        lower1(i // 2, i % 2 * 256, 256)

    @pl.loop(0, 2)
    def _(d):
        lower0(d, 768, HALF)
        lower1(d, 768, HALF)

    next(ob)

    def swapped_row(k, carry):
        v = csrc_ref[k]
        fc_ref[pl.ds(k, 1), left] = landed(oa_ref, v)
        fc_ref[pl.ds(k, 1), right] = landed(ob_ref, v)
        return carry

    lax.fori_loop(0, CAP, swapped_row, 0, unroll=8)
    both = pl.ds(0, 2 * NB)

    @pl.loop(0, 4)
    def _(i):
        cols = tile(i)
        u0 = dot3(inv(li_s, 0, full, full), split(t_ref[0:NB, cols]))
        put(u_s, full, cols, u0)
        for d in (0, 1):
            rows2 = pl.ds(NB + 256 * d, 256)
            t_ref[rows2, cols] = t_ref[rows2, cols] - dot3(
                get(l_s, lrow(d, NB, 256), full), get(u_s, full, cols))
        t1 = t_ref[NB:, cols]
        u1 = dot3(inv(li_s, 1, full, full), split(t1))
        put(u_s, pl.ds(NB, NB), cols, u1)

        @pl.loop(0, 4)
        def _(k):
            r = tile(k)
            f_ref[r, cols] = a_ref[pl.ds(k * 2, 2), :, :, cols].reshape(256, 256) - dot3(
                get(l_s, lrow(k // 2, k % 2 * 256, 256), both), get(u_s, both, cols))

        for d in (0, 1):
            r = pl.ds(d * HALF, HALF)
            fc_ref[r, cols] = fc_ref[r, cols] - dot3(
                get(l_s, lrow(d, 768, HALF), both), get(u_s, both, cols))

        @pl.when(p == 0)
        def _():
            f_ref[0:NB, cols] = u0

            @pl.when((c == 0) & (i < 2))
            def _():
                f_ref[0:NB, cols] = t_ref[0:NB, cols]

        @pl.when(p == 1)
        def _():
            f_ref[0:NB, cols] = u1

            @pl.when((c == 1) & (i < 2))
            def _():
                f_ref[0:NB, cols] = t1

    def joined(r, k):
        return l_s[0, r, k].astype(F32) + l_s[1, r, k].astype(F32)

    for j in range(2):
        part = pl.ds(j * NB, NB)

        @pl.when(c == j)
        def _():
            f_ref[NB:, left] = joined(lrow(1, 0, NB), part)
            for d in (0, 1):
                fc_ref[pl.ds(d * HALF, HALF), left] = joined(lrow(d, 768, HALF), part)

            @pl.when(p > j)
            def _():
                f_ref[0:NB, left] = joined(lrow(0, 0, NB), part)

    @pl.when((c == 0) & (p == 1))
    def _():
        for d in (0, 1):
            f_ref[pl.ds(256 * d, 256), left] = joined(lrow(d, NB, 256), full)

    for g in (sa, oa, sb, ob):
        next(g)
    scatter_drain(0)
    scatter_drain(1)
    z_drain()


def factor(pack, take, csrc, matrix, li, ui):
    dma = pltpu.SemaphoreType.DMA
    return pl.pallas_call(
        factor_kernel,
        out_shape=(
            jax.ShapeDtypeStruct((1024, 1024), F32),
            jax.ShapeDtypeStruct((CAP, 1024), F32),
        ),
        in_specs=[spec(SM)] * 3 + [spec(VM)] * 3,
        out_specs=(spec(VM), spec(VM)),
        scratch_shapes=[
            VM((16, CAP, NB), F32),
            VM((16, 2 * CHUNK, NB), F32),
            VM((16, CAP, NB), F32),
            VM((16, 2 * CHUNK, NB), F32),
            VM((2, 2, ROWS, NB), F32),
            VM((1024, 1024), F32),
            VM((2, 1024, 1024), BF16),
            VM((2, 2 * ROWS, 1024), BF16),
            VM((2, NB, NB), BF16),
            VM((4, NB, NB), BF16),
            VM((4, NB, NB), BF16),
            VM((2, 4, CHUNK, 256), F32),
            VM((2, 2, 4, CHUNK, 256), F32),
            dma((12,)), dma((2,)), dma((4,)), dma((24,)), dma((8,)), dma((8,)),
            dma((160,)), dma((160,)),
            dma((STREAM,)), dma((STREAM,)), dma((STREAM,)), dma((STREAM,)),
            dma((2 * STREAM,)), dma((2 * STREAM,)),
        ],
        compiler_params=pltpu.CompilerParams(collective_id=0, has_side_effects=True,
                                             vmem_limit_bytes=67043328),
        name="factor",
    )(pack, take, csrc, matrix.reshape(8, 4, CHUNK, 1024), li, ui)


def place_kernel(cpos_ref, count_ref, f_ref, fc_ref, o_ref):
    o_ref[...] = f_ref[...]

    def one(k, carry):
        o_ref[pl.ds(cpos_ref[k], 1), :] = fc_ref[pl.ds(k, 1), :]
        return carry

    lax.fori_loop(0, count_ref[0], one, 0)


def place(cpos, count, f, fc):
    return pl.pallas_call(
        place_kernel,
        out_shape=jax.ShapeDtypeStruct((1024, 1024), F32),
        in_specs=[spec(SM), spec(SM), spec(VM), spec(VM)],
        out_specs=spec(VM),
        name="place",
    )(cpos, count, f, fc)


def spread(value, axis, source):
    kept = jnp.where(lax.axis_index(axis) == source, value, 0).astype(value.dtype)
    return lax.psum(kept, axis)


def duplicate_kernel(a_ref, o_ref):
    o_ref[...] = a_ref[...]


def duplicate(matrix):
    return pl.pallas_call(
        duplicate_kernel, out_shape=jax.ShapeDtypeStruct(matrix.shape, F32),
        in_specs=[spec(VM)], out_specs=spec(VM), name="duplicate",
    )(matrix)


def general(matrix, pivots, lower_inverses, upper_inverses):
    my_row = lax.axis_index("prow")
    my_col = lax.axis_index("pcol")
    rows_local, cols_local = matrix.shape
    dot = functools.partial(jnp.dot, precision=lax.Precision.HIGH, preferred_element_type=F32)
    row_blocks = jnp.arange(rows_local, dtype=jnp.int32) // NB * 16 + my_row
    col_blocks = jnp.arange(cols_local, dtype=jnp.int32) // NB * 16 + my_col

    def panel(step, current):
        targets = pivots[step]
        blocks = targets // NB
        slot = blocks // 16 * NB + targets % NB
        is_mine = blocks % 16 == my_row
        picked = jnp.where(is_mine[:, None], current[slot], 0.0)
        old_top = spread(current[:NB], "prow", step)
        new_top = lax.psum(picked, "prow")
        after = (col_blocks > step)[None, :]
        top = jnp.where(after, dot(lower_inverses[step], new_top), new_top)
        current = current.at[jnp.where(is_mine, slot, rows_local)].set(old_top, mode="drop")
        current = current.at[:NB].set(jnp.where(my_row == step, top, current[:NB]))
        column = spread(current[:, :NB], "pcol", step)
        below = (row_blocks > step)[:, None]
        lower = jnp.where(below, dot(column, upper_inverses[step]), 0.0)
        current = current - dot(lower, jnp.where(after, top, 0.0))
        return current.at[:, :NB].set(
            jnp.where(below & (my_col == step), lower, current[:, :NB]))

    return lax.fori_loop(0, 2, panel, duplicate(matrix))


def body(matrix, pivots, lower_inverses, upper_inverses):
    pack, take, csrc, cpos, total, fits = tables(pivots, lax.axis_index("prow"))

    def fast():
        return place(cpos, total, *factor(pack, take, csrc, matrix,
                                          lower_inverses, upper_inverses))

    return lax.cond(
        fits, fast, lambda: general(matrix, pivots, lower_inverses, upper_inverses))


def solution(mesh):
    placed = (P("prow", "pcol"), P(), P(), P())
    return jax.shard_map(
        body, mesh=mesh, in_specs=placed, out_specs=P("prow", "pcol"), check_vma=False
    )
```

```python
import functools

import jax
import jax.numpy as jnp
from jax import lax
from jax.experimental import pallas as pl
from jax.experimental.pallas import tpu as pltpu
from jax.sharding import PartitionSpec as P

NB = 512
CAP = 96
CHUNK = 32
HALF = CAP // 2
ZROWS = 16
ROWS = 768 + HALF
STREAM = 768 // ZROWS
SKEW = 5
VM = pltpu.VMEM
SM = pltpu.SMEM
F32 = jnp.float32
BF16 = jnp.bfloat16


def spec(space):
    return pl.BlockSpec(memory_space=space)


def remote(src, dst, send, recv, where):
    return pltpu.make_async_remote_copy(
        src_ref=src, dst_ref=dst, send_sem=send, recv_sem=recv,
        device_id=where, device_id_type=pl.DeviceIdType.MESH,
    )


def tables(pivots, me):
    p0, p1 = pivots[0], pivots[1]
    i = jnp.arange(NB, dtype=jnp.int32)
    r = jnp.arange(2 * NB, dtype=jnp.int32)

    def held(rows, default):
        hit = jnp.max(jnp.where(rows[:, None] == p0[None, :], i[None, :] + 1, 0), axis=1)
        return jnp.where(hit > 0, hit - 1, default)

    t = jnp.concatenate([p0, held(p1, p1)])
    owner = (t >> 9) & 15
    local = ((t >> 13) << 9) | (t & 511)
    earlier = (owner[None, :] == owner[:, None]) & (r[None, :] < r[:, None])
    rank = jnp.sum(earlier.astype(jnp.int32), axis=1)
    k = jnp.arange(CAP, dtype=jnp.int32)
    mine = (owner == me)[None, :] & (rank[None, :] == k[:, None])
    pack = jnp.sum(jnp.where(mine, local[None, :], 0), axis=1)
    second = held(i + NB, i + NB)
    g = (((r >> 9) << 4) + me) * NB + (r & 511)
    m1 = jnp.max(jnp.where(g[:, None] == p1[None, :], second[None, :] + 1, 0), axis=1)
    m0 = jnp.max(jnp.where(g[:, None] == p0[None, :], i[None, :] + 1, 0), axis=1)
    src = jnp.where(g < 2 * NB, -1, jnp.where(m1 > 0, m1, m0) - 1)
    valid = src >= 0
    count = jnp.sum((valid[None, :] & (r[None, :] < r[:, None])).astype(jnp.int32), axis=1)
    chosen = valid[None, :] & (count[None, :] == k[:, None])
    cpos = jnp.sum(jnp.where(chosen, r[None, :], 0), axis=1)
    csrc = jnp.sum(jnp.where(chosen, src[None, :], 0), axis=1)
    came = (csrc & 511) >> 5, (csrc >> 9) * CHUNK + (csrc & 31)
    total = jnp.sum(valid.astype(jnp.int32)).reshape(1)
    return (pack, owner, rank) + came, cpos, total, jnp.max(rank) < CAP


def split(v):
    hi = v.astype(BF16)
    return hi, (v - hi.astype(F32)).astype(BF16)


def dot3(a, b):
    f = functools.partial(jnp.dot, preferred_element_type=F32)
    return f(a[0], b[0]) + (f(a[0], b[1]) + f(a[1], b[0]))


def put(ref, rows, cols, v):
    hi, lo = split(v)
    ref[0, rows, cols] = hi
    ref[1, rows, cols] = lo


def get(ref, rows, cols):
    return ref[0, rows, cols], ref[1, rows, cols]


def factor_kernel(pack_ref, tq_ref, tr_ref, cq_ref, cr_ref, a_ref, li_ref, ui_ref, f_ref, fc_ref,
                  sa_ref, oa_ref, sb_ref, ob_ref, pp_ref, t_ref, u_s, l_s, uc_s, li_s, ui_s, sta, stb,
                  sc_send, sca_recv, scb_recv, sc2_send, sc2_recv, loc_sem,
                  ag_send, ag_recv,
                  up_send, up_recv, dn_send, dn_recv, sib_send, sib_recv,
                  far_send, far_recv, pair_send, pair_recv):
    p = lax.axis_index("prow")
    x, y = p // 4, p % 4
    c = lax.axis_index("pcol")
    z, core = c // 2, c % 2

    def at(px, py):
        return {"prow": px * 4 + py}

    def zat(pz, pc):
        return {"pcol": pz * 2 + pc}

    def signal(sem, where):
        pl.semaphore_signal(sem, inc=1, device_id=where,
                            device_id_type=pl.DeviceIdType.MESH)

    barrier = pltpu.get_barrier_semaphore()
    for d in (1, 2, 3):
        signal(barrier, at((x + d) % 4, y))
        signal(barrier, at(x, (y + d) % 4))
    for d in range(1, 8):
        signal(barrier, zat((z + d) % 8, core))
    signal(barrier, zat(z, 1 - core))

    def packed_row(k, carry):
        l = pack_ref[k]
        row = a_ref[l // 128, (l // 32) % 4, pl.ds(l % 32, 1), :]
        sa_ref[p, pl.ds(k, 1), :] = row[:, 0:NB]
        sb_ref[p, pl.ds(k, 1), :] = row[:, NB:]
        return carry

    lax.fori_loop(0, CAP, packed_row, 0, unroll=4)

    @pl.when(z == 0)
    def _():
        @pl.loop(0, 32)
        def _(i):
            pp_ref[core, i // 16, pl.ds(pl.multiple_of(i % 16 * 32, 32), 32), :] = (
                a_ref[i // 4, i % 4, :, 0:NB])

    pl.semaphore_wait(barrier, 14)

    def quarter(i):
        return pl.ds(256 * i, 256)

    packed, olds = (sa_ref, sb_ref), (oa_ref, ob_ref)

    def old(panel):
        return pl.ds(panel * CHUNK, CHUNK)

    def first_a(ab, panel, d):
        k = (x + d) % 4
        return remote(a_ref.at[k, :, :, quarter(2 * ab)], sta.at[ab],
                      sc_send.at[ab * 6 + d - 1], sca_recv.at[ab], at(k, y))

    def first_b(ab, panel, d):
        k = (y + d) % 4
        return remote(a_ref.at[pl.ds(0, 4), k, :, quarter(2 * ab + 1)], stb.at[ab, panel],
                      sc_send.at[ab * 6 + d + 2], scb_recv.at[ab * 2 + panel], at(x, k))

    def second_a(ab, panel, d, src):
        k = (y + d) % 4
        return remote(src.at[k], olds[ab].at[x * 4 + k, old(panel), quarter(0)],
                      sc2_send.at[ab * 12 + panel * 6 + d - 1],
                      sc2_recv.at[ab * 4 + panel * 2], at(x, k))

    def second_b(ab, panel, d, src):
        k = (x + d) % 4
        return remote(src.at[k], olds[ab].at[k * 4 + y, old(panel), quarter(1)],
                      sc2_send.at[ab * 12 + panel * 6 + d + 2],
                      sc2_recv.at[ab * 4 + panel * 2 + 1], at(k, y))

    def own(ab, panel, half, src):
        return pltpu.make_async_copy(src, olds[ab].at[p, old(panel), quarter(half)],
                                     loc_sem.at[ab * 4 + panel * 2 + half])

    def scatter(ab):
        qa, qb = quarter(2 * ab), quarter(2 * ab + 1)
        for panel in range(2):
            @pl.when(p == panel)
            def _():
                for d in (2, 1, 3):
                    first_a(ab, panel, d).start()
                    first_b(ab, panel, d).start()
                for d in (2, 1, 3):
                    second_a(ab, panel, d, a_ref.at[0, :, :, qa]).start()
                    second_b(ab, panel, d, a_ref.at[pl.ds(0, 4), panel, :, qb]).start()
                own(ab, panel, 0, a_ref.at[0, panel, :, qa]).start()
                own(ab, panel, 1, a_ref.at[0, panel, :, qb]).start()

    def relay(ab):
        for panel in range(2):
            @pl.when((y == panel) & (x != 0))
            def _():
                first_a(ab, panel, 1).wait_recv()
                for d in (2, 1, 3):
                    second_a(ab, panel, d, sta.at[ab]).start()
                own(ab, panel, 0, sta.at[ab, panel]).start()

            @pl.when((x == 0) & (y != panel))
            def _():
                first_b(ab, panel, 1).wait_recv()
                for d in (2, 1, 3):
                    second_b(ab, panel, d, stb.at[ab, panel]).start()
                own(ab, panel, 1, stb.at[ab, panel, 0]).start()

    def scattered(ab):
        for panel in range(2):
            @pl.when(y == panel)
            def _():
                own(ab, panel, 0, sta.at[ab, panel]).wait()

            @pl.when(y != panel)
            def _():
                second_a(ab, panel, 1, sta.at[ab]).wait_recv()

            @pl.when(x == 0)
            def _():
                own(ab, panel, 1, stb.at[ab, panel, 0]).wait()

            @pl.when(x != 0)
            def _():
                second_b(ab, panel, 1, stb.at[ab, panel]).wait_recv()

    def scatter_drain(ab):
        for panel in range(2):
            @pl.when(p == panel)
            def _():
                for d in (1, 2, 3):
                    first_a(ab, panel, d).wait_send()
                    first_b(ab, panel, d).wait_send()

            @pl.when(y == panel)
            def _():
                for d in (1, 2, 3):
                    second_a(ab, panel, d, sta.at[ab]).wait_send()

            @pl.when(x == 0)
            def _():
                for d in (1, 2, 3):
                    second_b(ab, panel, d, stb.at[ab, panel]).wait_send()

    def coords(half, du, dv):
        if half == 0:
            return (x + du) % 4, (y + dv) % 4
        return (x + dv) % 4, (y + du) % 4

    shift = (0, 3, 1, 2)
    hs = (0, 1)

    def all_gather(ab, kind):
        n = (CAP, 2 * CHUNK)[kind]
        buffer = (packed, olds)[kind][ab]
        m = n // 2
        part = ab * 2 + kind

        def cp(half, slot, du, dv, r0, rows, tu, tv):
            bx, by = coords(half, du, dv)
            ref = buffer.at[bx * 4 + by, pl.ds(r0, rows), quarter(half)]
            s = (part * 2 + half) * 20 + slot
            return remote(ref, ref, ag_send.at[s], ag_recv.at[s], at(*coords(half, tu, tv)))

        def st1(half, which):
            return cp(half, which, *(
                (0, 0, 0, n, 1, 0),
                (0, 0, 0, n, 3, 0),
                (3, 0, 0, m, 1, 0),
                (1, 0, m, m, 3, 0),
            )[which])

        def st2(half, j, which):
            u = shift[j]
            return cp(half, 4 + j * 4 + which, *(
                (u, 0, 0, n, 0, 1),
                (u, 0, 0, n, 0, 3),
                (u, 3, 0, m, 0, 1),
                (u, 1, m, m, 0, 3),
            )[which])

        for h in hs:
            st1(h, 0).start()
            st1(h, 1).start()
        for h in hs:
            st2(h, 0, 0).start()
            st2(h, 0, 1).start()
        yield
        for h in hs:
            st1(h, 0).wait_recv()
            st1(h, 2).start()
            st1(h, 1).wait_recv()
            st1(h, 3).start()
        for h in hs:
            for j in (1, 2):
                st2(h, j, 0).start()
                st2(h, j, 1).start()
        yield
        for h in hs:
            st1(h, 2).wait_recv()
            st1(h, 3).wait_recv()
            st2(h, 3, 0).start()
            st2(h, 3, 1).start()
        yield
        for j in range(4):
            for h in hs:
                st2(h, j, 0).wait_recv()
                st2(h, j, 2).start()
                st2(h, j, 1).wait_recv()
                st2(h, j, 3).start()
        yield
        for j in range(4):
            for h in hs:
                st2(h, j, 2).wait_recv()
                st2(h, j, 3).wait_recv()
        yield
        for h in hs:
            for w in range(4):
                st1(h, w).wait_send()
                for j in range(4):
                    st2(h, j, w).wait_send()
        yield

    def rows(k):
        return pl.ds(pl.multiple_of(k * ZROWS, ZROWS), ZROWS)

    def hop(k, d):
        ref = pp_ref.at[core, d, rows(k)]
        if d == 0:
            return remote(ref, ref, up_send.at[k], up_recv.at[k], zat((z + 1) % 8, core))
        return remote(ref, ref, dn_send.at[k], dn_recv.at[k], zat((z + 7) % 8, core))

    def sib(k, d, which):
        ref = pp_ref.at[which, d, rows(k)]
        s = d * STREAM + k
        return remote(ref, ref, sib_send.at[s], sib_recv.at[s], zat(z, 1 - core))

    def z_source(k0, k1):
        def step(k, carry):
            for d in (0, 1):
                hop(k, d).start()
            for d in (0, 1):
                sib(k, d, core).start()
            return carry
        lax.fori_loop(k0, k1, step, 0)

    def z_relay(t0, t1):
        @pl.when(z != 0)
        def _():
            def step(t, carry):
                for d in (0, 1):
                    k = t - SKEW * (z if d == 0 else 8 - z)

                    @pl.when((k >= 0) & (k < STREAM))
                    def _():
                        hop(k, d).wait_recv()

                        @pl.when(z != (7 if d == 0 else 1))
                        def _():
                            hop(k, d).start()
                        sib(k, d, core).start()
                return carry
            lax.fori_loop(t0, t1, step, 0)

    def z_finish():
        def got(k, carry):
            for d in (0, 1):
                sib(k, d, 1 - core).wait_recv()
            return carry
        lax.fori_loop(0, STREAM, got, 0)

    def z_drain():
        def sent(k, carry):
            for d in (0, 1):
                sib(k, d, core).wait_send()

                @pl.when(z != (7 if d == 0 else 1))
                def _():
                    hop(k, d).wait_send()
            return carry
        lax.fori_loop(0, STREAM, sent, 0)

    def top(buffer, r):
        return buffer[tq_ref[r], pl.ds(tr_ref[r], 1), :]

    def came(buffer, k):
        return buffer[cq_ref[k], pl.ds(cr_ref[k], 1), :]

    left, right = pl.ds(0, NB), pl.ds(NB, NB)

    def panel_tops():
        @pl.when(z == 0)
        def _():
            def one(r, carry):
                pp_ref[core, r // 256, pl.ds(NB + r % 256, 1), :] = top(sa_ref, r + NB * (1 - core))
                return carry
            lax.fori_loop(0, NB, one, 0, unroll=8)
            z_source(32, 48)

    def panel_swapped():
        @pl.when(z == 0)
        def _():
            def one(k, carry):
                pp_ref[core, k // HALF, pl.ds(768 + k % HALF, 1), :] = came(oa_ref, k)
                return carry
            lax.fori_loop(0, CAP, one, 0, unroll=8)
            for d in (4, 3, 5, 2, 6, 1, 7):
                far(d).start()

    def swapped_part(which):
        return pp_ref.at[which, :, pl.ds(768, HALF), :]

    def far(d):
        ref = swapped_part(core)
        return remote(ref, ref, far_send.at[d - 1], far_recv.at[0], zat(d, core))

    def pair(which):
        ref = swapped_part(which)
        return remote(ref, ref, pair_send.at[0], pair_recv.at[0], zat(z, 1 - core))

    def swapped_pair():
        @pl.when(z != 0)
        def _():
            far(1).wait_recv()
        pair(core).start()

    sa, oa = all_gather(0, 0), all_gather(0, 1)
    sb, ob = all_gather(1, 0), all_gather(1, 1)
    next(sa)

    @pl.when(z == 0)
    def _():
        z_source(0, 32)

    for j in range(2):
        li_s[2 * j], li_s[2 * j + 1] = split(li_ref[j])
        ui_s[2 * j], ui_s[2 * j + 1] = split(ui_ref[j])
    z_relay(5, 9)
    next(sa)
    z_relay(9, 13)
    next(sa)
    scatter(0)
    z_relay(13, 23)
    next(sa)
    z_relay(23, 29)
    next(sa)
    panel_tops()
    next(sb)
    scatter(1)
    z_relay(29, 33)
    relay(0)
    z_relay(33, 42)
    scattered(0)
    next(oa)
    z_relay(42, 45)
    next(sb)
    z_relay(45, 50)
    next(oa)
    z_relay(50, 54)
    next(oa)
    next(sb)
    z_relay(54, 57)
    relay(1)
    z_relay(57, 62)
    next(oa)
    next(sb)
    z_relay(62, 70)
    next(oa)
    panel_swapped()
    z_relay(70, 76)
    next(sb)
    scattered(1)
    next(ob)
    z_relay(76, STREAM + 7 * SKEW)
    z_finish()

    full = pl.ds(0, NB)

    def tile(i, size=256):
        return pl.ds(pl.multiple_of(i * size, size), size)

    def lrow(d, r, n):
        return pl.ds(pl.multiple_of(d * ROWS + r, 16), n)

    def inv(ref, j, r, k):
        return ref[2 * j, r, k], ref[2 * j + 1, r, k]

    def top_row(r, carry):
        t_ref[pl.ds(r, 1), left] = top(sa_ref, r)
        t_ref[pl.ds(r, 1), right] = top(sb_ref, r)
        return carry

    lax.fori_loop(0, 2 * NB, top_row, 0, unroll=8)
    next(ob)

    def lower0(d, r, n):
        src = pl.ds(pl.multiple_of(r, 16), n)
        put(l_s, lrow(d, r, n), full, dot3(split(pp_ref[0, d, src, :]), inv(ui_s, 0, full, full)))

    def lower1(d, r, n):
        src = pl.ds(pl.multiple_of(r, 16), n)
        rest = pp_ref[1, d, src, :] - dot3(get(l_s, lrow(d, r, n), full), get(uc_s, full, full))
        put(l_s, lrow(d, r, n), pl.ds(NB, NB), dot3(split(rest), inv(ui_s, 1, full, full)))

    put(uc_s, full, full, sum(
        dot3(inv(li_s, 0, full, tile(d)), split(pp_ref[1, d, pl.ds(NB, 256), :]))
        for d in (0, 1)
    ))
    next(ob)

    @pl.loop(0, 2)
    def _(d):
        lower0(d, 0, 768)
        lower1(d, 0, 512)

    swapped_pair()
    next(ob)
    both = pl.ds(0, 2 * NB)

    @pl.loop(0, 4)
    def _(i):
        cols = tile(i)
        u0 = dot3(inv(li_s, 0, full, full), split(t_ref[0:NB, cols]))
        put(u_s, full, cols, u0)
        for d in (0, 1):
            rows2 = pl.ds(NB + 256 * d, 256)
            t_ref[rows2, cols] = t_ref[rows2, cols] - dot3(
                get(l_s, lrow(d, NB, 256), full), get(u_s, full, cols))
        t1 = t_ref[NB:, cols]
        u1 = dot3(inv(li_s, 1, full, full), split(t1))
        put(u_s, pl.ds(NB, NB), cols, u1)

        @pl.loop(0, 2)
        def _(k):
            r = tile(k, 512)
            f_ref[r, cols] = a_ref[pl.ds(k * 4, 4), :, :, cols].reshape(512, 256) - dot3(
                get(l_s, lrow(k, 0, 512), both), get(u_s, both, cols))

        @pl.when(p == 0)
        def _():
            f_ref[0:NB, cols] = u0

            @pl.when((c == 0) & (i < 2))
            def _():
                f_ref[0:NB, cols] = t_ref[0:NB, cols]

        @pl.when(p == 1)
        def _():
            f_ref[0:NB, cols] = u1

            @pl.when((c == 1) & (i < 2))
            def _():
                f_ref[0:NB, cols] = t1

    next(ob)

    def swapped_row(k, carry):
        fc_ref[pl.ds(k, 1), left] = came(oa_ref, k)
        fc_ref[pl.ds(k, 1), right] = came(ob_ref, k)
        return carry

    lax.fori_loop(0, CAP, swapped_row, 0, unroll=8)
    pair(1 - core).wait_recv()

    @pl.loop(0, 2)
    def _(d):
        lower0(d, 768, HALF)
        lower1(d, 768, HALF)

    @pl.loop(0, 4)
    def _(i):
        cols = tile(i)
        for d in (0, 1):
            r = pl.ds(d * HALF, HALF)
            fc_ref[r, cols] = fc_ref[r, cols] - dot3(
                get(l_s, lrow(d, 768, HALF), both), get(u_s, both, cols))

    def joined(r, k):
        return l_s[0, r, k].astype(F32) + l_s[1, r, k].astype(F32)

    for j in range(2):
        part = pl.ds(j * NB, NB)

        @pl.when(c == j)
        def _():
            f_ref[NB:, left] = joined(lrow(1, 0, NB), part)
            for d in (0, 1):
                fc_ref[pl.ds(d * HALF, HALF), left] = joined(lrow(d, 768, HALF), part)

            @pl.when(p > j)
            def _():
                f_ref[0:NB, left] = joined(lrow(0, 0, NB), part)

    @pl.when((c == 0) & (p == 1))
    def _():
        for d in (0, 1):
            f_ref[pl.ds(256 * d, 256), left] = joined(lrow(d, NB, 256), full)

    for g in (sa, oa, sb, ob):
        next(g)
    scatter_drain(0)
    scatter_drain(1)
    z_drain()
    pair(core).wait_send()

    @pl.when(z == 0)
    def _():
        for d in range(1, 8):
            far(d).wait_send()


def factor(rows, matrix, li, ui):
    dma = pltpu.SemaphoreType.DMA
    return pl.pallas_call(
        factor_kernel,
        out_shape=(
            jax.ShapeDtypeStruct((1024, 1024), F32),
            jax.ShapeDtypeStruct((CAP, 1024), F32),
        ),
        in_specs=[spec(SM)] * 5 + [spec(VM)] * 3,
        out_specs=(spec(VM), spec(VM)),
        scratch_shapes=[
            VM((16, CAP, NB), F32),
            VM((16, 2 * CHUNK, NB), F32),
            VM((16, CAP, NB), F32),
            VM((16, 2 * CHUNK, NB), F32),
            VM((2, 2, ROWS, NB), F32),
            VM((1024, 1024), F32),
            VM((2, 1024, 1024), BF16),
            VM((2, 2 * ROWS, 1024), BF16),
            VM((2, NB, NB), BF16),
            VM((4, NB, NB), BF16),
            VM((4, NB, NB), BF16),
            VM((2, 4, CHUNK, 256), F32),
            VM((2, 2, 4, CHUNK, 256), F32),
            dma((12,)), dma((2,)), dma((4,)), dma((24,)), dma((8,)), dma((8,)),
            dma((160,)), dma((160,)),
            dma((STREAM,)), dma((STREAM,)), dma((STREAM,)), dma((STREAM,)),
            dma((2 * STREAM,)), dma((2 * STREAM,)),
            dma((7,)), dma((1,)), dma((1,)), dma((1,)),
        ],
        compiler_params=pltpu.CompilerParams(collective_id=0, has_side_effects=True,
                                             vmem_limit_bytes=67043328),
        name="factor",
    )(*rows, matrix.reshape(8, 4, CHUNK, 1024), li, ui)


def place_kernel(cpos_ref, count_ref, f_ref, fc_ref, o_ref):
    o_ref[...] = f_ref[...]

    def one(k, carry):
        o_ref[pl.ds(cpos_ref[k], 1), :] = fc_ref[pl.ds(k, 1), :]
        return carry

    lax.fori_loop(0, count_ref[0], one, 0)


def place(cpos, count, f, fc):
    return pl.pallas_call(
        place_kernel,
        out_shape=jax.ShapeDtypeStruct((1024, 1024), F32),
        in_specs=[spec(SM), spec(SM), spec(VM), spec(VM)],
        out_specs=spec(VM),
        name="place",
    )(cpos, count, f, fc)


def ring_sum(value, axis):
    ring = [(i, (i + 1) % 16) for i in range(16)]

    def step(_, carry):
        total, moving = carry
        moving = lax.ppermute(moving, axis, ring)
        return total + moving, moving

    return lax.fori_loop(0, 15, step, (value, value))[0]


def spread(value, axis, source):
    return ring_sum(jnp.where(lax.axis_index(axis) == source, value, 0.0), axis)


def duplicate_kernel(a_ref, o_ref):
    o_ref[...] = a_ref[...]


def duplicate(matrix):
    return pl.pallas_call(
        duplicate_kernel, out_shape=jax.ShapeDtypeStruct(matrix.shape, F32),
        in_specs=[spec(VM)], out_specs=spec(VM), name="duplicate",
    )(matrix)


def general(matrix, pivots, lower_inverses, upper_inverses):
    my_row = lax.axis_index("prow")
    my_col = lax.axis_index("pcol")
    rows_local, cols_local = matrix.shape
    dot = functools.partial(jnp.dot, precision=lax.Precision.HIGH, preferred_element_type=F32)
    row_blocks = jnp.arange(rows_local, dtype=jnp.int32) // NB * 16 + my_row
    col_blocks = jnp.arange(cols_local, dtype=jnp.int32) // NB * 16 + my_col

    def panel(step, current):
        targets = pivots[step]
        blocks = targets // NB
        slot = blocks // 16 * NB + targets % NB
        is_mine = blocks % 16 == my_row
        picked = jnp.where(is_mine[:, None], current[slot], 0.0)
        old_top = spread(current[:NB], "prow", step)
        new_top = ring_sum(picked, "prow")
        after = (col_blocks > step)[None, :]
        top = jnp.where(after, dot(lower_inverses[step], new_top), new_top)
        current = current.at[jnp.where(is_mine, slot, rows_local)].set(old_top, mode="drop")
        current = current.at[:NB].set(jnp.where(my_row == step, top, current[:NB]))
        column = spread(current[:, :NB], "pcol", step)
        below = (row_blocks > step)[:, None]
        lower = jnp.where(below, dot(column, upper_inverses[step]), 0.0)
        current = current - dot(lower, jnp.where(after, top, 0.0))
        return current.at[:, :NB].set(
            jnp.where(below & (my_col == step), lower, current[:, :NB]))

    return lax.fori_loop(0, 2, panel, duplicate(matrix))


def body(matrix, pivots, lower_inverses, upper_inverses):
    rows, cpos, total, fits = tables(pivots, lax.axis_index("prow"))

    def fast():
        return place(cpos, total, *factor(rows, matrix, lower_inverses, upper_inverses))

    return lax.cond(
        fits, fast, lambda: general(matrix, pivots, lower_inverses, upper_inverses))


def solution(mesh):
    placed = (P("prow", "pcol"), P(), P(), P())
    return jax.shard_map(
        body, mesh=mesh, in_specs=placed, out_specs=P("prow", "pcol"), check_vma=False
    )
```

```python
import functools

import jax
import jax.numpy as jnp
from jax import lax
from jax.experimental import pallas as pl
from jax.experimental.pallas import tpu as pltpu
from jax.sharding import PartitionSpec as P

NB = 512
CAP = 96
CHUNK = 32
HALF = CAP // 2
ZROWS = 16
ROWS = 768 + HALF
STREAM = 768 // ZROWS
SKEW = 5
VM = pltpu.VMEM
SM = pltpu.SMEM
F32 = jnp.float32
BF16 = jnp.bfloat16


def spec(space):
    return pl.BlockSpec(memory_space=space)


def remote(src, dst, send, recv, where):
    return pltpu.make_async_remote_copy(
        src_ref=src, dst_ref=dst, send_sem=send, recv_sem=recv,
        device_id=where, device_id_type=pl.DeviceIdType.MESH,
    )


def tables(pivots, me):
    p0, p1 = pivots[0], pivots[1]
    i = jnp.arange(NB, dtype=jnp.int32)
    r = jnp.arange(2 * NB, dtype=jnp.int32)

    def held(rows, default):
        hit = jnp.max(jnp.where(rows[:, None] == p0[None, :], i[None, :] + 1, 0), axis=1)
        return jnp.where(hit > 0, hit - 1, default)

    t = jnp.concatenate([p0, held(p1, p1)])
    owner = (t >> 9) & 15
    local = ((t >> 13) << 9) | (t & 511)
    earlier = (owner[None, :] == owner[:, None]) & (r[None, :] < r[:, None])
    rank = jnp.sum(earlier.astype(jnp.int32), axis=1)
    k = jnp.arange(CAP, dtype=jnp.int32)
    mine = (owner == me)[None, :] & (rank[None, :] == k[:, None])
    pack = jnp.sum(jnp.where(mine, local[None, :], 0), axis=1)
    second = held(i + NB, i + NB)
    g = (((r >> 9) << 4) + me) * NB + (r & 511)
    m1 = jnp.max(jnp.where(g[:, None] == p1[None, :], second[None, :] + 1, 0), axis=1)
    m0 = jnp.max(jnp.where(g[:, None] == p0[None, :], i[None, :] + 1, 0), axis=1)
    src = jnp.where(g < 2 * NB, -1, jnp.where(m1 > 0, m1, m0) - 1)
    valid = src >= 0
    count = jnp.sum((valid[None, :] & (r[None, :] < r[:, None])).astype(jnp.int32), axis=1)
    chosen = valid[None, :] & (count[None, :] == k[:, None])
    cpos = jnp.sum(jnp.where(chosen, r[None, :], 0), axis=1)
    csrc = jnp.sum(jnp.where(chosen, src[None, :], 0), axis=1)
    came = (csrc & 511) >> 5, (csrc >> 9) * CHUNK + (csrc & 31)
    total = jnp.sum(valid.astype(jnp.int32)).reshape(1)
    return (pack, owner, rank) + came, cpos, total, jnp.max(rank) < CAP


def split(v):
    hi = v.astype(BF16)
    return hi, (v - hi.astype(F32)).astype(BF16)


def dot3(a, b):
    f = functools.partial(jnp.dot, preferred_element_type=F32)
    return f(a[0], b[0]) + (f(a[0], b[1]) + f(a[1], b[0]))


def put(ref, rows, cols, v):
    hi, lo = split(v)
    ref[0, rows, cols] = hi
    ref[1, rows, cols] = lo


def get(ref, rows, cols):
    return ref[0, rows, cols], ref[1, rows, cols]


def factor_kernel(pack_ref, tq_ref, tr_ref, cq_ref, cr_ref, a_ref, li_ref, ui_ref, f_ref, fc_ref,
                  sa_ref, oa_ref, sb_ref, ob_ref, pp_ref, t_ref, u_s, l_s, uc_s, li_s, ui_s, sta, stb,
                  sc_send, sca_recv, scb_recv, sc2_send, sc2_recv, loc_sem,
                  ag_send, ag_recv,
                  up_send, up_recv, dn_send, dn_recv, sib_send, sib_recv,
                  far_send, far_recv, pair_send, pair_recv):
    p = lax.axis_index("prow")
    x, y = p // 4, p % 4
    c = lax.axis_index("pcol")
    z, core = c // 2, c % 2

    def at(px, py):
        return {"prow": px * 4 + py}

    def zat(pz, pc):
        return {"pcol": pz * 2 + pc}

    def signal(sem, where):
        pl.semaphore_signal(sem, inc=1, device_id=where,
                            device_id_type=pl.DeviceIdType.MESH)

    barrier = pltpu.get_barrier_semaphore()
    for d in (1, 2, 3):
        signal(barrier, at((x + d) % 4, y))
        signal(barrier, at(x, (y + d) % 4))
    for d in range(1, 8):
        signal(barrier, zat((z + d) % 8, core))
    signal(barrier, zat(z, 1 - core))

    def packed_row(k, carry):
        l = pack_ref[k]
        row = a_ref[l // 128, (l // 32) % 4, pl.ds(l % 32, 1), :]
        sa_ref[p, pl.ds(k, 1), :] = row[:, 0:NB]
        sb_ref[p, pl.ds(k, 1), :] = row[:, NB:]
        return carry

    lax.fori_loop(0, CAP, packed_row, 0, unroll=4)

    @pl.when(z == 0)
    def _():
        @pl.loop(0, 32)
        def _(i):
            pp_ref[core, i // 16, pl.ds(pl.multiple_of(i % 16 * 32, 32), 32), :] = (
                a_ref[i // 4, i % 4, :, 0:NB])

    pl.semaphore_wait(barrier, 14)

    def quarter(i):
        return pl.ds(256 * i, 256)

    packed, olds = (sa_ref, sb_ref), (oa_ref, ob_ref)

    def old(panel):
        return pl.ds(panel * CHUNK, CHUNK)

    def first_a(ab, panel, d):
        k = (x + d) % 4
        return remote(a_ref.at[k, :, :, quarter(2 * ab)], sta.at[ab],
                      sc_send.at[ab * 6 + d - 1], sca_recv.at[ab], at(k, y))

    def first_b(ab, panel, d):
        k = (y + d) % 4
        return remote(a_ref.at[pl.ds(0, 4), k, :, quarter(2 * ab + 1)], stb.at[ab, panel],
                      sc_send.at[ab * 6 + d + 2], scb_recv.at[ab * 2 + panel], at(x, k))

    def second_a(ab, panel, d, src):
        k = (y + d) % 4
        return remote(src.at[k], olds[ab].at[x * 4 + k, old(panel), quarter(0)],
                      sc2_send.at[ab * 12 + panel * 6 + d - 1],
                      sc2_recv.at[ab * 4 + panel * 2], at(x, k))

    def second_b(ab, panel, d, src):
        k = (x + d) % 4
        return remote(src.at[k], olds[ab].at[k * 4 + y, old(panel), quarter(1)],
                      sc2_send.at[ab * 12 + panel * 6 + d + 2],
                      sc2_recv.at[ab * 4 + panel * 2 + 1], at(k, y))

    def own(ab, panel, half, src):
        return pltpu.make_async_copy(src, olds[ab].at[p, old(panel), quarter(half)],
                                     loc_sem.at[ab * 4 + panel * 2 + half])

    def scatter(ab):
        qa, qb = quarter(2 * ab), quarter(2 * ab + 1)
        for panel in range(2):
            @pl.when(p == panel)
            def _():
                for d in (2, 1, 3):
                    first_a(ab, panel, d).start()
                    first_b(ab, panel, d).start()
                for d in (2, 1, 3):
                    second_a(ab, panel, d, a_ref.at[0, :, :, qa]).start()
                    second_b(ab, panel, d, a_ref.at[pl.ds(0, 4), panel, :, qb]).start()
                own(ab, panel, 0, a_ref.at[0, panel, :, qa]).start()
                own(ab, panel, 1, a_ref.at[0, panel, :, qb]).start()

    def relay(ab):
        for panel in range(2):
            @pl.when((y == panel) & (x != 0))
            def _():
                first_a(ab, panel, 1).wait_recv()
                for d in (2, 1, 3):
                    second_a(ab, panel, d, sta.at[ab]).start()
                own(ab, panel, 0, sta.at[ab, panel]).start()

            @pl.when((x == 0) & (y != panel))
            def _():
                first_b(ab, panel, 1).wait_recv()
                for d in (2, 1, 3):
                    second_b(ab, panel, d, stb.at[ab, panel]).start()
                own(ab, panel, 1, stb.at[ab, panel, 0]).start()

    def scattered(ab):
        for panel in range(2):
            @pl.when(y == panel)
            def _():
                own(ab, panel, 0, sta.at[ab, panel]).wait()

            @pl.when(y != panel)
            def _():
                second_a(ab, panel, 1, sta.at[ab]).wait_recv()

            @pl.when(x == 0)
            def _():
                own(ab, panel, 1, stb.at[ab, panel, 0]).wait()

            @pl.when(x != 0)
            def _():
                second_b(ab, panel, 1, stb.at[ab, panel]).wait_recv()

    def scatter_drain(ab):
        for panel in range(2):
            @pl.when(p == panel)
            def _():
                for d in (1, 2, 3):
                    first_a(ab, panel, d).wait_send()
                    first_b(ab, panel, d).wait_send()

            @pl.when(y == panel)
            def _():
                for d in (1, 2, 3):
                    second_a(ab, panel, d, sta.at[ab]).wait_send()

            @pl.when(x == 0)
            def _():
                for d in (1, 2, 3):
                    second_b(ab, panel, d, stb.at[ab, panel]).wait_send()

    def coords(half, du, dv):
        if half == 0:
            return (x + du) % 4, (y + dv) % 4
        return (x + dv) % 4, (y + du) % 4

    shift = (0, 3, 1, 2)
    hs = (0, 1)

    def all_gather(ab, kind):
        n = (CAP, 2 * CHUNK)[kind]
        buffer = (packed, olds)[kind][ab]
        m = n // 2
        part = ab * 2 + kind

        def cp(half, slot, du, dv, r0, rows, tu, tv):
            bx, by = coords(half, du, dv)
            ref = buffer.at[bx * 4 + by, pl.ds(r0, rows), quarter(half)]
            s = (part * 2 + half) * 20 + slot
            return remote(ref, ref, ag_send.at[s], ag_recv.at[s], at(*coords(half, tu, tv)))

        def st1(half, which):
            return cp(half, which, *(
                (0, 0, 0, n, 1, 0),
                (0, 0, 0, n, 3, 0),
                (3, 0, 0, m, 1, 0),
                (1, 0, m, m, 3, 0),
            )[which])

        def st2(half, j, which):
            u = shift[j]
            return cp(half, 4 + j * 4 + which, *(
                (u, 0, 0, n, 0, 1),
                (u, 0, 0, n, 0, 3),
                (u, 3, 0, m, 0, 1),
                (u, 1, m, m, 0, 3),
            )[which])

        for h in hs:
            st1(h, 0).start()
            st1(h, 1).start()
        for h in hs:
            st2(h, 0, 0).start()
            st2(h, 0, 1).start()
        yield
        for h in hs:
            st1(h, 0).wait_recv()
            st1(h, 2).start()
            st1(h, 1).wait_recv()
            st1(h, 3).start()
        for h in hs:
            for j in (1, 2):
                st2(h, j, 0).start()
                st2(h, j, 1).start()
        yield
        for h in hs:
            st1(h, 2).wait_recv()
            st1(h, 3).wait_recv()
            st2(h, 3, 0).start()
            st2(h, 3, 1).start()
        yield
        for j in range(4):
            for h in hs:
                st2(h, j, 0).wait_recv()
                st2(h, j, 2).start()
                st2(h, j, 1).wait_recv()
                st2(h, j, 3).start()
        yield
        for j in range(4):
            for h in hs:
                st2(h, j, 2).wait_recv()
                st2(h, j, 3).wait_recv()
        yield
        for h in hs:
            for w in range(4):
                st1(h, w).wait_send()
                for j in range(4):
                    st2(h, j, w).wait_send()
        yield

    def rows(k):
        return pl.ds(pl.multiple_of(k * ZROWS, ZROWS), ZROWS)

    def hop(k, d):
        ref = pp_ref.at[core, d, rows(k)]
        if d == 0:
            return remote(ref, ref, up_send.at[k], up_recv.at[k], zat((z + 1) % 8, core))
        return remote(ref, ref, dn_send.at[k], dn_recv.at[k], zat((z + 7) % 8, core))

    def sib(k, d, which):
        ref = pp_ref.at[which, d, rows(k)]
        s = d * STREAM + k
        return remote(ref, ref, sib_send.at[s], sib_recv.at[s], zat(z, 1 - core))

    def z_source(k0, k1):
        def step(k, carry):
            for d in (0, 1):
                hop(k, d).start()
            for d in (0, 1):
                sib(k, d, core).start()
            return carry
        lax.fori_loop(k0, k1, step, 0)

    def z_relay(t0, t1):
        @pl.when(z != 0)
        def _():
            def step(t, carry):
                for d in (0, 1):
                    k = t - SKEW * (z if d == 0 else 8 - z)

                    @pl.when((k >= 0) & (k < STREAM))
                    def _():
                        hop(k, d).wait_recv()

                        @pl.when(z != (7 if d == 0 else 1))
                        def _():
                            hop(k, d).start()
                        sib(k, d, core).start()
                return carry
            lax.fori_loop(t0, t1, step, 0)

    def z_finish():
        def got(k, carry):
            for d in (0, 1):
                sib(k, d, 1 - core).wait_recv()
            return carry
        lax.fori_loop(0, STREAM, got, 0)

    def z_drain():
        def sent(k, carry):
            for d in (0, 1):
                sib(k, d, core).wait_send()

                @pl.when(z != (7 if d == 0 else 1))
                def _():
                    hop(k, d).wait_send()
            return carry
        lax.fori_loop(0, STREAM, sent, 0)

    def top(buffer, r):
        return buffer[tq_ref[r], pl.ds(tr_ref[r], 1), :]

    def came(buffer, k):
        return buffer[cq_ref[k], pl.ds(cr_ref[k], 1), :]

    left, right = pl.ds(0, NB), pl.ds(NB, NB)

    def panel_tops():
        @pl.when(z == 0)
        def _():
            def one(r, carry):
                pp_ref[core, r // 256, pl.ds(NB + r % 256, 1), :] = top(sa_ref, r + NB * (1 - core))
                return carry
            lax.fori_loop(0, NB, one, 0, unroll=8)
            z_source(32, 48)

    def panel_swapped():
        @pl.when(z == 0)
        def _():
            def one(k, carry):
                pp_ref[core, k // HALF, pl.ds(768 + k % HALF, 1), :] = came(oa_ref, k)
                return carry
            lax.fori_loop(0, CAP, one, 0, unroll=8)
            for d in (4, 3, 5, 2, 6, 1, 7):
                far(d).start()

    def swapped_part(which):
        return pp_ref.at[which, :, pl.ds(768, HALF), :]

    def far(d):
        ref = swapped_part(core)
        return remote(ref, ref, far_send.at[d - 1], far_recv.at[0], zat(d, core))

    def pair(which):
        ref = swapped_part(which)
        return remote(ref, ref, pair_send.at[0], pair_recv.at[0], zat(z, 1 - core))

    def swapped_pair():
        @pl.when(z != 0)
        def _():
            far(1).wait_recv()
        pair(core).start()

    sa, oa = all_gather(0, 0), all_gather(0, 1)
    sb, ob = all_gather(1, 0), all_gather(1, 1)
    next(sa)

    @pl.when(z == 0)
    def _():
        z_source(0, 32)

    for j in range(2):
        li_s[2 * j], li_s[2 * j + 1] = split(li_ref[j])
        ui_s[2 * j], ui_s[2 * j + 1] = split(ui_ref[j])
    z_relay(5, 9)
    next(sa)
    z_relay(9, 13)
    next(sa)
    scatter(0)
    z_relay(13, 23)
    next(sa)
    z_relay(23, 29)
    next(sa)
    panel_tops()
    next(sb)
    scatter(1)
    z_relay(29, 33)
    relay(0)
    z_relay(33, 42)
    scattered(0)
    next(oa)
    z_relay(42, 45)
    next(sb)
    z_relay(45, 50)
    next(oa)
    z_relay(50, 54)
    next(oa)
    next(sb)
    z_relay(54, 57)
    relay(1)
    z_relay(57, 62)
    next(oa)
    next(sb)
    z_relay(62, 70)
    next(oa)
    panel_swapped()
    z_relay(70, STREAM + 7 * SKEW)
    z_finish()

    full = pl.ds(0, NB)

    def tile(i, size=256):
        return pl.ds(pl.multiple_of(i * size, size), size)

    def lrow(d, r, n):
        return pl.ds(pl.multiple_of(d * ROWS + r, 16), n)

    def inv(ref, j, r, k):
        return ref[2 * j, r, k], ref[2 * j + 1, r, k]

    def lower0(d, r, n):
        src = pl.ds(pl.multiple_of(r, 16), n)
        put(l_s, lrow(d, r, n), full, dot3(split(pp_ref[0, d, src, :]), inv(ui_s, 0, full, full)))

    def lower1(d, r, n):
        src = pl.ds(pl.multiple_of(r, 16), n)
        rest = pp_ref[1, d, src, :] - dot3(get(l_s, lrow(d, r, n), full), get(uc_s, full, full))
        put(l_s, lrow(d, r, n), pl.ds(NB, NB), dot3(split(rest), inv(ui_s, 1, full, full)))

    put(uc_s, full, full, sum(
        dot3(inv(li_s, 0, full, tile(d)), split(pp_ref[1, d, pl.ds(NB, 256), :]))
        for d in (0, 1)
    ))
    next(sb)
    scattered(1)
    next(ob)
    lower0(0, 0, 768)
    lower1(0, 0, 512)
    next(ob)
    lower0(1, 0, 768)
    lower1(1, 0, 512)
    next(ob)
    swapped_pair()

    def top_row(r, carry):
        t_ref[pl.ds(r, 1), left] = top(sa_ref, r)
        t_ref[pl.ds(r, 1), right] = top(sb_ref, r)
        return carry

    lax.fori_loop(0, 2 * NB, top_row, 0, unroll=8)
    next(ob)
    both = pl.ds(0, 2 * NB)

    @pl.loop(0, 4)
    def _(i):
        cols = tile(i)
        u0 = dot3(inv(li_s, 0, full, full), split(t_ref[0:NB, cols]))
        put(u_s, full, cols, u0)
        for d in (0, 1):
            rows2 = pl.ds(NB + 256 * d, 256)
            t_ref[rows2, cols] = t_ref[rows2, cols] - dot3(
                get(l_s, lrow(d, NB, 256), full), get(u_s, full, cols))
        t1 = t_ref[NB:, cols]
        u1 = dot3(inv(li_s, 1, full, full), split(t1))
        put(u_s, pl.ds(NB, NB), cols, u1)

        @pl.loop(0, 2)
        def _(k):
            r = tile(k, 512)
            f_ref[r, cols] = a_ref[pl.ds(k * 4, 4), :, :, cols].reshape(512, 256) - dot3(
                get(l_s, lrow(k, 0, 512), both), get(u_s, both, cols))

        @pl.when(p == 0)
        def _():
            f_ref[0:NB, cols] = u0

            @pl.when((c == 0) & (i < 2))
            def _():
                f_ref[0:NB, cols] = t_ref[0:NB, cols]

        @pl.when(p == 1)
        def _():
            f_ref[0:NB, cols] = u1

            @pl.when((c == 1) & (i < 2))
            def _():
                f_ref[0:NB, cols] = t1

    next(ob)

    def swapped_row(k, carry):
        fc_ref[pl.ds(k, 1), left] = came(oa_ref, k)
        fc_ref[pl.ds(k, 1), right] = came(ob_ref, k)
        return carry

    lax.fori_loop(0, CAP, swapped_row, 0, unroll=8)
    pair(1 - core).wait_recv()

    @pl.loop(0, 2)
    def _(d):
        lower0(d, 768, HALF)
        lower1(d, 768, HALF)

    @pl.loop(0, 4)
    def _(i):
        cols = tile(i)
        for d in (0, 1):
            r = pl.ds(d * HALF, HALF)
            fc_ref[r, cols] = fc_ref[r, cols] - dot3(
                get(l_s, lrow(d, 768, HALF), both), get(u_s, both, cols))

    def joined(r, k):
        return l_s[0, r, k].astype(F32) + l_s[1, r, k].astype(F32)

    for j in range(2):
        part = pl.ds(j * NB, NB)

        @pl.when(c == j)
        def _():
            f_ref[NB:, left] = joined(lrow(1, 0, NB), part)
            for d in (0, 1):
                fc_ref[pl.ds(d * HALF, HALF), left] = joined(lrow(d, 768, HALF), part)

            @pl.when(p > j)
            def _():
                f_ref[0:NB, left] = joined(lrow(0, 0, NB), part)

    @pl.when((c == 0) & (p == 1))
    def _():
        for d in (0, 1):
            f_ref[pl.ds(256 * d, 256), left] = joined(lrow(d, NB, 256), full)

    for g in (sa, oa, sb, ob):
        next(g)
    scatter_drain(0)
    scatter_drain(1)
    z_drain()
    pair(core).wait_send()

    @pl.when(z == 0)
    def _():
        for d in range(1, 8):
            far(d).wait_send()


def factor(rows, matrix, li, ui):
    dma = pltpu.SemaphoreType.DMA
    return pl.pallas_call(
        factor_kernel,
        out_shape=(
            jax.ShapeDtypeStruct((1024, 1024), F32),
            jax.ShapeDtypeStruct((CAP, 1024), F32),
        ),
        in_specs=[spec(SM)] * 5 + [spec(VM)] * 3,
        out_specs=(spec(VM), spec(VM)),
        scratch_shapes=[
            VM((16, CAP, NB), F32),
            VM((16, 2 * CHUNK, NB), F32),
            VM((16, CAP, NB), F32),
            VM((16, 2 * CHUNK, NB), F32),
            VM((2, 2, ROWS, NB), F32),
            VM((1024, 1024), F32),
            VM((2, 1024, 1024), BF16),
            VM((2, 2 * ROWS, 1024), BF16),
            VM((2, NB, NB), BF16),
            VM((4, NB, NB), BF16),
            VM((4, NB, NB), BF16),
            VM((2, 4, CHUNK, 256), F32),
            VM((2, 2, 4, CHUNK, 256), F32),
            dma((12,)), dma((2,)), dma((4,)), dma((24,)), dma((8,)), dma((8,)),
            dma((160,)), dma((160,)),
            dma((STREAM,)), dma((STREAM,)), dma((STREAM,)), dma((STREAM,)),
            dma((2 * STREAM,)), dma((2 * STREAM,)),
            dma((7,)), dma((1,)), dma((1,)), dma((1,)),
        ],
        compiler_params=pltpu.CompilerParams(collective_id=0, has_side_effects=True,
                                             vmem_limit_bytes=67043328),
        name="factor",
    )(*rows, matrix.reshape(8, 4, CHUNK, 1024), li, ui)


def place_kernel(cpos_ref, count_ref, f_ref, fc_ref, o_ref):
    o_ref[...] = f_ref[...]

    def one(k, carry):
        o_ref[pl.ds(cpos_ref[k], 1), :] = fc_ref[pl.ds(k, 1), :]
        return carry

    lax.fori_loop(0, count_ref[0], one, 0)


def place(cpos, count, f, fc):
    return pl.pallas_call(
        place_kernel,
        out_shape=jax.ShapeDtypeStruct((1024, 1024), F32),
        in_specs=[spec(SM), spec(SM), spec(VM), spec(VM)],
        out_specs=spec(VM),
        name="place",
    )(cpos, count, f, fc)


def ring_sum(value, axis):
    ring = [(i, (i + 1) % 16) for i in range(16)]

    def step(_, carry):
        total, moving = carry
        moving = lax.ppermute(moving, axis, ring)
        return total + moving, moving

    return lax.fori_loop(0, 15, step, (value, value))[0]


def spread(value, axis, source):
    return ring_sum(jnp.where(lax.axis_index(axis) == source, value, 0.0), axis)


def duplicate_kernel(a_ref, o_ref):
    o_ref[...] = a_ref[...]


def duplicate(matrix):
    return pl.pallas_call(
        duplicate_kernel, out_shape=jax.ShapeDtypeStruct(matrix.shape, F32),
        in_specs=[spec(VM)], out_specs=spec(VM), name="duplicate",
    )(matrix)


def general(matrix, pivots, lower_inverses, upper_inverses):
    my_row = lax.axis_index("prow")
    my_col = lax.axis_index("pcol")
    rows_local, cols_local = matrix.shape
    dot = functools.partial(jnp.dot, precision=lax.Precision.HIGH, preferred_element_type=F32)
    row_blocks = jnp.arange(rows_local, dtype=jnp.int32) // NB * 16 + my_row
    col_blocks = jnp.arange(cols_local, dtype=jnp.int32) // NB * 16 + my_col

    def panel(step, current):
        targets = pivots[step]
        blocks = targets // NB
        slot = blocks // 16 * NB + targets % NB
        is_mine = blocks % 16 == my_row
        picked = jnp.where(is_mine[:, None], current[slot], 0.0)
        old_top = spread(current[:NB], "prow", step)
        new_top = ring_sum(picked, "prow")
        after = (col_blocks > step)[None, :]
        top = jnp.where(after, dot(lower_inverses[step], new_top), new_top)
        current = current.at[jnp.where(is_mine, slot, rows_local)].set(old_top, mode="drop")
        current = current.at[:NB].set(jnp.where(my_row == step, top, current[:NB]))
        column = spread(current[:, :NB], "pcol", step)
        below = (row_blocks > step)[:, None]
        lower = jnp.where(below, dot(column, upper_inverses[step]), 0.0)
        current = current - dot(lower, jnp.where(after, top, 0.0))
        return current.at[:, :NB].set(
            jnp.where(below & (my_col == step), lower, current[:, :NB]))

    return lax.fori_loop(0, 2, panel, duplicate(matrix))


def body(matrix, pivots, lower_inverses, upper_inverses):
    rows, cpos, total, fits = tables(pivots, lax.axis_index("prow"))

    def fast():
        return place(cpos, total, *factor(rows, matrix, lower_inverses, upper_inverses))

    return lax.cond(
        fits, fast, lambda: general(matrix, pivots, lower_inverses, upper_inverses))


def solution(mesh):
    placed = (P("prow", "pcol"), P(), P(), P())
    return jax.shard_map(
        body, mesh=mesh, in_specs=placed, out_specs=P("prow", "pcol"), check_vma=False
    )
```
